32 devices in a mesh: gx: 4 (over z), gy: 4 (over y, x), gz: 2 (over core).
Axes of the slice: x: 2, y: 2, z: 4, core: 2. Of those that a mesh axis runs over, the one named last changes fastest.
Arguments:
- right_side: float32 [64, 64, 32, 256], P('gx', 'gy', 'gz'), may hold values from -35 to 35
- conductivity: float32 [64, 64, 32], P('gx', 'gy', 'gz'), may hold values from 0.25 to 2
- reaction: float32 [64, 64, 32], P('gx', 'gy', 'gz'), may hold values from 0.25 to 4
- leaf_factor: float32 [8, 8, 4, 512, 512], P('gx', 'gy', 'gz'), as said below
- leaf_weight: float32 [8, 8, 4, 512, 64], P('gx', 'gy', 'gz'), may hold values from -0.25 to 0.25
- leaf_skeleton: int32 [8, 8, 4, 64], P('gx', 'gy', 'gz'), may hold values from 0 to 511, as said below
- device_factor: float32 [4, 4, 2, 512, 512], P('gx', 'gy', 'gz'), as said below
- device_weight: float32 [4, 4, 2, 512, 256], P('gx', 'gy', 'gz'), may hold values from -0.25 to 0.25
- device_skeleton: int32 [4, 4, 2, 256], P('gx', 'gy', 'gz'), may hold values from 0 to 511, as said below
- column_factor: float32 [4, 4, 512, 512], P('gx', 'gy', 'gz'), as said below
- column_weight: float32 [4, 4, 512, 128], P('gx', 'gy'), may hold values from -0.25 to 0.25
- column_skeleton: int32 [4, 4, 128], P('gx', 'gy'), may hold values from 0 to 511, as said below
- top_factor: float32 [2048, 2048], P(('gx', 'gy')), as said below
Outputs:
- solution: float32 [64, 64, 32, 256], P('gx', 'gy', 'gz')
The draws below stay inside these ranges and needn't reach their ends.
Inputs may be any that keep to these rules, and one draw needn't show every extreme that they name: `leaf_factor`: each box's block is symmetric and positive definite. `device_factor`: each domain block's block is symmetric and positive definite. `column_factor`: each column's block is symmetric and positive definite. `top_factor`: symmetric and positive definite. `leaf_skeleton`: the 64 numbers of one box are all different. `device_skeleton`: the 256 numbers of one domain block are all different. `column_skeleton`: the 128 numbers of one column are all different.
All inputs are finite; a program needn't handle non-finite values.
Results may differ from the reference program's by a relative error of at most 0.0001.
Values sent between devices are 32-bit elements; how exact they have to be, the bound alone decides.
No kernel may reach another device: no remote copies, remote signals or barrier semaphores. Data moves between devices by JAX's collectives and lax.ppermute only.
A program may use at most 128 MiB of HBM per device.

```python
import math
import jax
import jax.numpy as jnp
from jax import lax

BLOCK = 16
BOX = 8
NRHS = 256
K0 = 64
K1 = 256
K2 = 128
ITERS = 2
LEAF = 512
R1 = 512
R2 = 512
R_TOP = 2048
NX = 64
NY = 64
NZ = 32
NBX = 8
NBY = 8
NBZ = 4
N_GX = 4
N_GY = 4
N_GZ = 2


def symmetric_dominant(key, shape):
    dimension = shape[-1]
    first, second = jax.random.split(key)
    entries = jax.random.uniform(first, shape, jnp.float32, -0.25, 1.0)
    entries = 0.5 * (entries + jnp.swapaxes(entries, -1, -2))
    diagonal = jax.random.uniform(second, shape[:-1], jnp.float32, 1.2, 2.4)
    identity = jnp.eye(dimension, dtype=jnp.float32)
    return entries / dimension * (1.0 - identity) + identity * diagonal[..., None]


def skeleton_draw(key, leading, choices, count):
    full_shape = leading + (choices,)
    scores = jax.random.randint(key, full_shape, 0, 262144)
    scores = scores * choices + lax.broadcasted_iota(jnp.int32, full_shape, len(leading))
    ranked = jnp.argsort(scores, axis=-1, stable=True)
    return ranked[..., :count].astype(jnp.int32)


def draw_right_side(key, part):
    full_shape = (NX, NY, NZ, NRHS)
    place_x = lax.broadcasted_iota(jnp.float32, full_shape, 0) / max(NX - 1, 1)
    amplitude = 4.0 + 6.0 * place_x
    return jnp.clip(jax.random.normal(key, full_shape, jnp.float32), -3.5, 3.5) * amplitude


def draw_leaf_factor(key, part):
    return symmetric_dominant(jax.random.fold_in(key, 11), (NBX, NBY, NBZ, LEAF, LEAF))


def draw_device_factor(key, part):
    return symmetric_dominant(jax.random.fold_in(key, 12), (N_GX, N_GY, N_GZ, R1, R1))


def draw_column_factor(key, part):
    return symmetric_dominant(jax.random.fold_in(key, 13), (N_GX, N_GY, R2, R2))


def draw_top_factor(key, part):
    return symmetric_dominant(jax.random.fold_in(key, 14), (R_TOP, R_TOP))


def draw_leaf_skeleton(key, part):
    return skeleton_draw(jax.random.fold_in(key, 21), (NBX, NBY, NBZ), LEAF, K0)


def draw_device_skeleton(key, part):
    return skeleton_draw(jax.random.fold_in(key, 22), (N_GX, N_GY, N_GZ), R1, K1)


def draw_column_skeleton(key, part):
    return skeleton_draw(jax.random.fold_in(key, 23), (N_GX, N_GY), R2, K2)


def level_of(rng, extent, shards, smallest, largest):
    loudness, own = 1.0, jax.random.fold_in(rng, 6)
    for dim, parts in shards:
        heights = jnp.exp(jax.random.uniform(jax.random.fold_in(own, dim), (parts,), jnp.float32, smallest / len(shards), largest / len(shards)))
        loudness = loudness * jnp.repeat(heights, extent[dim] // parts).reshape([-1 if axis == dim else 1 for axis in range(len(extent))])
    return loudness


def scatter_about(own_key, dims, width, bound, shards=(), kind=jnp.bfloat16):
    array = width * jax.random.normal(own_key, dims, jnp.float32)
    if shards:
        array = array * level_of(own_key, dims, shards, -0.22, 0.18)
    return jnp.clip(array, -bound, bound).astype(kind)


def setup_inputs(seed: int = 0) -> dict:
    arg_keys = jax.random.split(jax.random.key(seed), 14)
    right_side = draw_right_side(jax.random.fold_in(arg_keys[13], 71), 0)
    conductivity = jnp.clip(jnp.exp(math.log(2.0) - 2.0794415 * jax.random.uniform(arg_keys[1], (NX, NY, NZ), jnp.float32) ** level_of(arg_keys[1], (NX, NY, NZ), ((0, 4), (1, 4), (2, 2)), -0.2, 0.2)), 0.25, 2.0)
    reaction = jnp.clip(jnp.exp(math.log(4.0) - 2.7725887 * jax.random.uniform(arg_keys[2], (NX, NY, NZ), jnp.float32) ** level_of(arg_keys[2], (NX, NY, NZ), ((0, 4), (1, 4), (2, 2)), -0.2, 0.2)), 0.25, 4.0)
    leaf_factor = draw_leaf_factor(jax.random.fold_in(arg_keys[13], 71), 0)
    leaf_weight = scatter_about(arg_keys[4], (NBX, NBY, NBZ, LEAF, K0), LEAF ** -0.5, 0.25, ((0, 4), (1, 4), (2, 2)), jnp.float32)
    leaf_skeleton = draw_leaf_skeleton(jax.random.fold_in(arg_keys[13], 71), 0)
    device_factor = draw_device_factor(jax.random.fold_in(arg_keys[13], 71), 0)
    device_weight = scatter_about(arg_keys[7], (N_GX, N_GY, N_GZ, R1, K1), R1 ** -0.5, 0.25, ((0, 4), (1, 4), (2, 2)), jnp.float32)
    device_skeleton = draw_device_skeleton(jax.random.fold_in(arg_keys[13], 71), 0)
    column_factor = draw_column_factor(jax.random.fold_in(arg_keys[13], 71), 0)
    column_weight = scatter_about(arg_keys[10], (N_GX, N_GY, R2, K2), R2 ** -0.5, 0.25, ((0, 4), (1, 4)), jnp.float32)
    column_skeleton = draw_column_skeleton(jax.random.fold_in(arg_keys[13], 71), 0)
    top_factor = draw_top_factor(jax.random.fold_in(arg_keys[13], 71), 0)
    return dict(right_side=right_side, conductivity=conductivity, reaction=reaction, leaf_factor=leaf_factor, leaf_weight=leaf_weight, leaf_skeleton=leaf_skeleton, device_factor=device_factor, device_weight=device_weight, device_skeleton=device_skeleton, column_factor=column_factor, column_weight=column_weight, column_skeleton=column_skeleton, top_factor=top_factor)


highest = lax.Precision.HIGHEST


def neighbour_slices():
    listing = []
    for axis_number in (0, 1, 2):
        for upper in (True, False):
            picked = [slice(1, -1), slice(1, -1), slice(1, -1)]
            picked[axis_number] = slice(2, None) if upper else slice(0, -2)
            listing.append(tuple(picked))
    return listing


def apply_operator(vector_field, conductivity, reaction):
    padded_cond = jnp.pad(conductivity, 1)
    padded_field = jnp.pad(vector_field, ((1, 1), (1, 1), (1, 1), (0, 0)))
    result = reaction[..., None] * vector_field
    for picked in neighbour_slices():
        coefficient = (0.5 * (conductivity + padded_cond[picked]))[..., None]
        result = result + coefficient * (vector_field - padded_field[picked])
    return result


def pick_rows(values, skeleton):
    leading = skeleton.shape[:-1]
    flat_values = values.reshape((-1,) + values.shape[-2:])
    flat_index = skeleton.reshape((-1, skeleton.shape[-1]))
    chosen = jax.vmap(lambda matrix, rows_index: matrix[rows_index])(flat_values, flat_index)
    return chosen.reshape(leading + chosen.shape[-2:])


def place_rows(values, skeleton, row_count):
    leading = skeleton.shape[:-1]
    flat_values = values.reshape((-1,) + values.shape[-2:])
    flat_index = skeleton.reshape((-1, skeleton.shape[-1]))

    def place_one(matrix, rows_index):
        return jnp.zeros((row_count, matrix.shape[-1]), matrix.dtype).at[rows_index].add(matrix)

    placed = jax.vmap(place_one)(flat_values, flat_index)
    return placed.reshape(leading + placed.shape[-2:])


def restrict(values, skeleton, weight):
    return pick_rows(values, skeleton) + jnp.einsum("...rk,...rn->...kn", weight, values, precision=highest)


def lift(coarse, skeleton, weight, row_count):
    return place_rows(coarse, skeleton, row_count) + jnp.einsum("...rk,...kn->...rn", weight, coarse, precision=highest)


def precondition(residual, leaf_factor, leaf_weight, leaf_skeleton, device_factor, device_weight, device_skeleton, column_factor, column_weight, column_skeleton, top_factor):
    systems = residual.shape[-1]
    per_side = BLOCK // BOX
    leaf_size = BOX * BOX * BOX
    boxes_x = NX // BOX
    boxes_y = NY // BOX
    boxes_z = NZ // BOX
    leaf_values = residual.reshape(boxes_x, BOX, boxes_y, BOX, boxes_z, BOX, systems).transpose(0, 2, 4, 1, 3, 5, 6).reshape(boxes_x, boxes_y, boxes_z, leaf_size, systems)
    leaf_up = restrict(leaf_values, leaf_skeleton, leaf_weight)
    device_values = leaf_up.reshape(N_GX, per_side, N_GY, per_side, N_GZ, per_side, K0, systems).transpose(0, 2, 4, 1, 3, 5, 6, 7).reshape(N_GX, N_GY, N_GZ, R1, systems)
    device_up = restrict(device_values, device_skeleton, device_weight)
    column_values = device_up.reshape(N_GX, N_GY, R2, systems)
    column_up = restrict(column_values, column_skeleton, column_weight)
    top_values = column_up.reshape(R_TOP, systems)
    top_result = jnp.dot(top_factor, top_values, precision=highest)
    column_result = jnp.einsum("abrm,abmn->abrn", column_factor, column_values, precision=highest) + lift(top_result.reshape(N_GX, N_GY, K2, systems), column_skeleton, column_weight, R2)
    device_result = jnp.einsum("abcrm,abcmn->abcrn", device_factor, device_values, precision=highest) + lift(column_result.reshape(N_GX, N_GY, N_GZ, K1, systems), device_skeleton, device_weight, R1)
    leaf_coarse = device_result.reshape(N_GX, N_GY, N_GZ, per_side, per_side, per_side, K0, systems).transpose(0, 3, 1, 4, 2, 5, 6, 7).reshape(boxes_x, boxes_y, boxes_z, K0, systems)
    leaf_result = jnp.einsum("abclm,abcmn->abcln", leaf_factor, leaf_values, precision=highest) + lift(leaf_coarse, leaf_skeleton, leaf_weight, leaf_size)
    return leaf_result.reshape(boxes_x, boxes_y, boxes_z, BOX, BOX, BOX, systems).transpose(0, 3, 1, 4, 2, 5, 6).reshape(NX, NY, NZ, systems)


def reference(right_side, conductivity, reaction, leaf_factor, leaf_weight, leaf_skeleton, device_factor, device_weight, device_skeleton, column_factor, column_weight, column_skeleton, top_factor):
    def smoothing(values):
        return precondition(values, leaf_factor, leaf_weight, leaf_skeleton, device_factor, device_weight, device_skeleton, column_factor, column_weight, column_skeleton, top_factor)

    solution = jnp.zeros_like(right_side)
    residual = right_side
    corrected = smoothing(residual)
    direction = corrected
    energy = jnp.sum(residual * corrected, axis=(0, 1, 2))
    for iteration in range(ITERS):
        applied = apply_operator(direction, conductivity, reaction)
        step_length = energy / jnp.sum(direction * applied, axis=(0, 1, 2))
        solution = solution + step_length * direction
        residual = residual - step_length * applied
        if iteration + 1 < ITERS:
            corrected = smoothing(residual)
            energy_new = jnp.sum(residual * corrected, axis=(0, 1, 2))
            direction = corrected + (energy_new / energy) * direction
            energy = energy_new
    return solution
```

```python
import functools

import jax
import jax.numpy as jnp
from jax import lax
from jax.experimental import pallas as pl
from jax.experimental.pallas import tpu as pltpu
from jax.sharding import PartitionSpec as P

BOX = 8
LANES = 128
MIB = 1 << 20

highest = lax.Precision.HIGHEST


def halves(values):
    high = values.astype(jnp.bfloat16)
    return high, (values - high.astype(values.dtype)).astype(jnp.bfloat16)


def product(left, right, left_dim=1):
    left_high, left_low = left if isinstance(left, tuple) else halves(left)
    right_high, right_low = right if isinstance(right, tuple) else halves(right)

    def one(a, b):
        return lax.dot_general(
            a, b, (((left_dim,), (0,)), ((), ())), preferred_element_type=jnp.float32
        )

    return one(left_high, right_high) + (one(left_low, right_high) + one(left_high, right_low))


def folded(weight, skeleton, first=0):
    rows = lax.broadcasted_iota(jnp.int32, weight.shape, weight.ndim - 2) + first
    return weight + (rows == skeleton).astype(weight.dtype)


def box_place(index, per_side):
    return index // (per_side * per_side), index // per_side % per_side, index % per_side


def cost(flops, moved):
    return pl.CostEstimate(flops=flops, bytes_accessed=moved, transcendentals=0)


def restrict_body(field, leaf_w, leaf_s, dev_w, dev_s, device_in, device_up):
    box = pl.program_id(0)
    systems = field.shape[-1]
    values = field[...].reshape(-1, systems)
    up = product(folded(leaf_w[0], leaf_s[0]), values, 0)
    device_in[...] = up
    rows = dev_w.shape[0]
    part = product(folded(dev_w[...], dev_s[...], box * rows), up, 0)

    @pl.when(box == 0)
    def _():
        device_up[...] = part

    @pl.when(box > 0)
    def _():
        device_up[...] += part


def restrict(field, leaf_w, leaf_s, dev_w, dev_s):
    boxes, leaf_size, kept = leaf_w.shape
    per_side = field.shape[0] // BOX
    systems = field.shape[-1]
    whole = boxes * kept
    dev_kept = dev_w.shape[1]
    return pl.pallas_call(
        restrict_body,
        grid=(boxes,),
        in_specs=[
            pl.BlockSpec((BOX, BOX, BOX, systems), lambda i: box_place(i, per_side) + (0,)),
            pl.BlockSpec((1, leaf_size, kept), lambda i: (i, 0, 0)),
            pl.BlockSpec((1, 1, kept), lambda i: (i, 0, 0)),
            pl.BlockSpec((kept, dev_kept), lambda i: (i, 0)),
            pl.BlockSpec((1, dev_kept), lambda i: (0, 0)),
        ],
        out_specs=[
            pl.BlockSpec((kept, systems), lambda i: (i, 0)),
            pl.BlockSpec((dev_kept, systems), lambda i: (0, 0)),
        ],
        out_shape=[
            jax.ShapeDtypeStruct((whole, systems), jnp.float32),
            jax.ShapeDtypeStruct((dev_kept, systems), jnp.float32),
        ],
        compiler_params=pltpu.CompilerParams(vmem_limit_bytes=16 * MIB),
        cost_estimate=cost(6 * systems * whole * (leaf_size + dev_kept), 4 * field.size),
        name="restrict",
    )(field, leaf_w, leaf_s, dev_w, dev_s)


def near_body(field, leaf_f, dev_f, device_in, col_f, column_in, leaf_near, dev_near, col_near):
    values = field[...]
    leaf_near[...] = product(leaf_f[0], values.reshape(-1, values.shape[-1])).reshape(values.shape)

    @pl.when(pl.program_id(0) == 0)
    def _():
        dev_near[...] = product(dev_f[...], device_in[...])
        col_near[...] = product(col_f[...], column_in[...])


def near(field, leaf_f, dev_f, device_in, col_f, column_in):
    boxes, leaf_size, _ = leaf_f.shape
    per_side = field.shape[0] // BOX
    systems = field.shape[-1]

    def whole(array):
        return pl.BlockSpec(array.shape, lambda i: (0, 0))

    cells = pl.BlockSpec((BOX, BOX, BOX, systems), lambda i: box_place(i, per_side) + (0,))
    out_shape = [
        jax.ShapeDtypeStruct(field.shape, jnp.float32),
        jax.ShapeDtypeStruct((dev_f.shape[0], systems), jnp.float32),
        jax.ShapeDtypeStruct((col_f.shape[0], systems), jnp.float32),
    ]
    return pl.pallas_call(
        near_body,
        grid=(boxes,),
        in_specs=[
            cells,
            pl.BlockSpec((1, leaf_size, leaf_size), lambda i: (i, 0, 0)),
            whole(dev_f),
            whole(device_in),
            whole(col_f),
            whole(column_in),
        ],
        out_specs=[cells, whole(out_shape[1]), whole(out_shape[2])],
        out_shape=out_shape,
        compiler_params=pltpu.CompilerParams(vmem_limit_bytes=20 * MIB),
        cost_estimate=cost(
            6 * systems * (leaf_f.size + dev_f.size + col_f.size), 4 * (leaf_f.size + 2 * field.size)
        ),
        name="near",
    )(field, leaf_f, dev_f, device_in, col_f, column_in)


def lift_body(update, top_out, col_w, col_s, first, col_near, dev_w, dev_s, dev_near, leaf_w, leaf_s, leaf_near, *rest):
    if update:
        base, step = rest[:2]
        rest = rest[2:]
    out, x_low, x_top, y_low, y_top, z_low, z_top, coarse = rest
    boxes, leaf_size, kept = leaf_w.shape
    cells = out.shape[0]
    systems = out.shape[-1]
    per_side = cells // BOX
    column_out = col_near[...] + product(folded(col_w[...], col_s[...], first[0]), top_out[...])
    device_out = dev_near[...] + product(folded(dev_w[...], dev_s[...]), column_out)
    coarse[...] = device_out.reshape(coarse.shape)

    def one_box(box, carry):
        a, b, c = box_place(box, per_side)
        here = (
            pl.ds(pl.multiple_of(a * BOX, BOX), BOX),
            pl.ds(pl.multiple_of(b * BOX, BOX), BOX),
            pl.ds(pl.multiple_of(c * BOX, BOX), BOX),
        )
        x, y, z = here
        far = product(folded(leaf_w[box], leaf_s[box]), coarse[box])
        values = leaf_near[here] + far.reshape(BOX, BOX, BOX, systems)
        if update:
            values = base[here] - step[...] * values
        out[here] = values

        @pl.when(a == 0)
        def _():
            x_low[y, z] = values[0]

        @pl.when(a == per_side - 1)
        def _():
            x_top[y, z] = values[BOX - 1]

        @pl.when(b == 0)
        def _():
            y_low[x, z] = values[:, 0]

        @pl.when(b == per_side - 1)
        def _():
            y_top[x, z] = values[:, BOX - 1]

        @pl.when(c == 0)
        def _():
            z_low[x, y] = values[:, :, 0]

        @pl.when(c == per_side - 1)
        def _():
            z_top[x, y] = values[:, :, BOX - 1]

        return carry

    lax.fori_loop(0, boxes, one_box, 0)


def lift(top_out, col_w, col_s, first, col_near, dev_w, dev_s, dev_near, leaf_w, leaf_s, leaf_near, extra=()):
    boxes, leaf_size, kept = leaf_w.shape
    systems = leaf_near.shape[-1]
    vmem = pl.BlockSpec(memory_space=pltpu.VMEM)
    face = jax.ShapeDtypeStruct(leaf_near.shape[1:], jnp.float32)
    return pl.pallas_call(
        functools.partial(lift_body, bool(extra)),
        in_specs=[vmem] * 3 + [pl.BlockSpec(memory_space=pltpu.SMEM)] + [vmem] * (7 + len(extra)),
        out_specs=[vmem] * 7,
        out_shape=[jax.ShapeDtypeStruct(leaf_near.shape, jnp.float32)] + [face] * 6,
        scratch_shapes=[pltpu.VMEM((boxes, kept, systems), jnp.float32)],
        compiler_params=pltpu.CompilerParams(vmem_limit_bytes=30 * MIB),
        cost_estimate=cost(6 * systems * (leaf_w.size + dev_w.size), 8 * leaf_near.size),
        name="lift",
    )(top_out, col_w, col_s, first, col_near, dev_w, dev_s, dev_near, leaf_w, leaf_s, leaf_near, *extra)


def spread_body(x_face, y_face, z_low, z_top, diagonal, *outs):
    for source, out in zip((x_face, y_face, z_low, z_top, diagonal), outs):

        def plane(x, carry, source=source, out=out):
            values = source[x]
            for y in range(out.shape[1]):
                out[x, y] = jnp.broadcast_to(values[:, y : y + 1], out.shape[2:])
            return carry

        lax.fori_loop(0, out.shape[0], plane, 0)


def spread(*sources):
    shapes = [jax.ShapeDtypeStruct((s.shape[0], s.shape[2], s.shape[1], LANES), jnp.float32) for s in sources]
    vmem = pl.BlockSpec(memory_space=pltpu.VMEM)
    return pl.pallas_call(
        spread_body,
        in_specs=[vmem] * len(sources),
        out_specs=[vmem] * len(sources),
        out_shape=shapes,
        compiler_params=pltpu.CompilerParams(vmem_limit_bytes=20 * MIB),
        cost_estimate=cost(sum(4 * s.size * LANES for s in sources), sum(4 * s.size * LANES for s in sources)),
        name="spread",
    )(*sources)


def stencil_plane(x, wide, field, below, above, y_below, y_above, z_below, z_above, coefs, sides):
    x_face, y_face, z_low, z_top, diagonal = coefs
    cells = field.shape[1]
    depth = field.shape[2]
    results = []
    rows = lax.broadcasted_iota(jnp.int32, (depth, field.shape[-1]), 0)
    for y in range(cells):
        here = field[x, y]
        total = wide(diagonal[x, y]) * here
        total -= wide(x_face[x, y]) * below(y)
        upper = above(y)
        if upper is not None:
            total -= wide(x_face[x + 1, y]) * upper
        total -= wide(y_face[x, y]) * (field[x, y - 1] if y else sides * y_below[x])
        if y < cells - 1:
            total -= wide(y_face[x, y + 1]) * field[x, y + 1]
        elif y_above is not None:
            total -= wide(y_face[x, y + 1]) * y_above[x]
        first = sides * z_below[x, pl.ds(y, 1)]
        lower = jnp.where(rows == 0, first, pltpu.roll(here, 1, 0))
        total -= wide(z_low[x, y]) * lower
        last = z_above[x, pl.ds(y, 1)] if z_above is not None else jnp.zeros_like(first)
        upper = jnp.where(rows == depth - 1, last, pltpu.roll(here, depth - 1, 0))
        total -= wide(z_top[x, y]) * upper
        results.append((here, total))
    return results


def sweep(field, x_halo, y_halo, z_halo, coefs, sides, use):
    cells = field.shape[0]
    systems = field.shape[-1]

    def wide(values):
        return jnp.concatenate([values] * (systems // LANES), axis=-1)

    def run(x, below, above):
        return stencil_plane(x, wide, field, below, above, *y_halo, *z_halo, coefs, sides)

    inside = lambda x: (lambda y: field[x, y])
    last = (lambda y: x_halo[1][y]) if x_halo[1] is not None else (lambda y: None)
    use(0, run(0, lambda y: sides * x_halo[0][y], inside(1)))

    def middle(x, carry):
        use(x, run(x, inside(x - 1), inside(x + 1)))
        return carry

    lax.fori_loop(1, cells - 1, middle, 0)
    use(cells - 1, run(cells - 1, inside(cells - 2), last))


def fold_rows(values):
    return values.reshape(-1, BOX, values.shape[-1]).sum(0)


def operator_body(field, xl, xt, yl, yt, zl, zt, cx, cy, cl, ct, cd, right, leaf_w, leaf_s, dev_w, dev_s, image, device_in, device_up, sums, parts):
    systems = field.shape[-1]
    cells = field.shape[0]
    per_side = cells // BOX
    parts[...] = jnp.zeros_like(parts)

    def use(x, results):
        energy = parts[0]
        curvature = parts[1]
        for y, (here, total) in enumerate(results):
            image[x, y] = total
            energy += fold_rows(right[x, y] * here)
            curvature += fold_rows(here * total)
        parts[0] = energy
        parts[1] = curvature

    sweep(field, (xl, xt), (yl, yt), (zl, zt), (cx, cy, cl, ct, cd), 1.0, use)
    sums[...] = jnp.concatenate(
        [parts[0].sum(0, keepdims=True), parts[1].sum(0, keepdims=True), jnp.zeros((BOX - 2, systems), jnp.float32)]
    )
    boxes, leaf_size, kept = leaf_w.shape
    device_up[...] = jnp.zeros_like(device_up)

    def one_box(box, carry):
        a, b, c = box_place(box, per_side)
        values = image[
            pl.ds(pl.multiple_of(a * BOX, BOX), BOX),
            pl.ds(pl.multiple_of(b * BOX, BOX), BOX),
            pl.ds(pl.multiple_of(c * BOX, BOX), BOX),
        ].reshape(-1, systems)
        up = product(folded(leaf_w[box], leaf_s[box]), values, 0)
        rows = pl.ds(pl.multiple_of(box * kept, kept), kept)
        device_in[rows] = up
        device_up[...] += product(folded(dev_w[rows], dev_s[...], box * kept), up, 0)
        return carry

    lax.fori_loop(0, boxes, one_box, 0)


def operator(field, halo, coefs, right, leaf_w, leaf_s, dev_w, dev_s):
    boxes, leaf_size, kept = leaf_w.shape
    systems = field.shape[-1]
    vmem = pl.BlockSpec(memory_space=pltpu.VMEM)
    ins = (field, *halo, *coefs, right, leaf_w, leaf_s, dev_w, dev_s)
    return pl.pallas_call(
        operator_body,
        in_specs=[vmem] * len(ins),
        out_specs=[vmem] * 4,
        out_shape=[
            jax.ShapeDtypeStruct(field.shape, jnp.float32),
            jax.ShapeDtypeStruct((boxes * kept, systems), jnp.float32),
            jax.ShapeDtypeStruct((dev_w.shape[1], systems), jnp.float32),
            jax.ShapeDtypeStruct((BOX, systems), jnp.float32),
        ],
        scratch_shapes=[pltpu.VMEM((2, BOX, systems), jnp.float32)],
        compiler_params=pltpu.CompilerParams(vmem_limit_bytes=40 * MIB),
        cost_estimate=cost(6 * systems * leaf_w.size + 60 * field.size, 16 * field.size),
        name="operator",
    )(*ins)


def forms_body(field, xl, yl, zl, cx, cy, cl, ct, cd, right, image, step, sums, parts):
    systems = field.shape[-1]
    parts[...] = jnp.zeros_like(parts)

    def use(x, results):
        energy = parts[0]
        curvature = parts[1]
        for y, (here, total) in enumerate(results):
            energy += fold_rows((right[x, y] - step[...] * image[x, y]) * here)
            curvature += fold_rows(here * total)
        parts[0] = energy
        parts[1] = curvature

    sweep(field, (xl, None), (yl, None), (zl, None), (cx, cy, cl, ct, cd), 2.0, use)
    sums[...] = jnp.concatenate(
        [parts[0].sum(0, keepdims=True), parts[1].sum(0, keepdims=True), jnp.zeros((BOX - 2, systems), jnp.float32)]
    )


def forms(field, halo, coefs, right, image, step):
    systems = field.shape[-1]
    vmem = pl.BlockSpec(memory_space=pltpu.VMEM)
    ins = (field, *halo, *coefs, right, image, step)
    return pl.pallas_call(
        forms_body,
        in_specs=[vmem] * len(ins),
        out_specs=vmem,
        out_shape=jax.ShapeDtypeStruct((BOX, systems), jnp.float32),
        scratch_shapes=[pltpu.VMEM((2, BOX, systems), jnp.float32)],
        compiler_params=pltpu.CompilerParams(vmem_limit_bytes=40 * MIB),
        cost_estimate=cost(60 * field.size, 12 * field.size),
        name="forms",
    )(*ins)


def shifted(values, axis, step):
    count = lax.axis_size(axis)
    return lax.ppermute(values, axis, [(i, (i + step) % count) for i in range(count)])


def from_below(top, axis):
    return lax.ppermute(top, axis, [(i, i + 1) for i in range(lax.axis_size(axis) - 1)])


def exchange(low, top, axis):
    if lax.axis_size(axis) == 2:
        other = lax.ppermute(jnp.where(lax.axis_index(axis) == 0, top, low), axis, [(0, 1), (1, 0)])
        return other, other
    above = lax.ppermute(low, axis, [(i + 1, i) for i in range(lax.axis_size(axis) - 1)])
    return from_below(top, axis), above


def local(
    right_side,
    conductivity,
    reaction,
    leaf_factor,
    leaf_weight,
    leaf_skeleton,
    device_factor,
    device_weight,
    device_skeleton,
    column_factor,
    column_weight,
    column_skeleton,
    top_factor,
):
    cells = right_side.shape[0]
    systems = right_side.shape[3]
    per_side = cells // BOX
    boxes = per_side**3
    leaf_size = BOX**3
    count_x, count_y, count_z = (lax.axis_size(a) for a in ("gx", "gy", "gz"))
    ix, iy, iz = (lax.axis_index(a) for a in ("gx", "gy", "gz"))
    leaf_f = leaf_factor.reshape(boxes, leaf_size, leaf_size)
    leaf_w = leaf_weight.reshape(boxes, leaf_size, -1)
    leaf_s = leaf_skeleton.reshape(boxes, 1, -1)
    dev_f = device_factor[0, 0, 0]
    dev_w = device_weight[0, 0, 0]
    dev_s = device_skeleton[0, 0]
    col_f = column_factor[0, 0]
    col_w = column_weight[0, 0]
    col_s = column_skeleton[0]
    rows_mine = dev_w.shape[1]
    col_k = col_w.shape[1]
    first_row = iz * rows_mine
    col_v = folded(col_w, col_s)
    col_w_mine = lax.dynamic_slice_in_dim(col_w, first_row, rows_mine, 0)
    part = systems // count_z
    split = part % LANES == 0
    if not split:
        part = systems

    blocks = top_factor.reshape(col_k, count_x, count_y, col_k)
    order = [(ix - k) % count_x for k in range(count_x)]
    top_blocks = []
    for k in range(count_y):
        chosen = lax.dynamic_index_in_dim(blocks, (iy + k) % count_y, 2, keepdims=False)
        moved = shifted(chosen, "gy", k) if k else chosen
        top_blocks.append(
            jnp.concatenate(
                [lax.dynamic_index_in_dim(moved, o, 1, keepdims=False) for o in order], axis=1
            )
        )
    top_block = jnp.concatenate(top_blocks, axis=0)

    def top_level(column_up, sums):
        gathered = [(column_up, sums)]
        mine = column_up if sums is None else jnp.concatenate([column_up, sums])
        for k in range(1, count_x):
            packed = shifted(mine, "gx", k)
            gathered.append((packed[:col_k], packed[col_k:]))
        partial = jnp.dot(top_block, jnp.concatenate([g[0] for g in gathered]), precision=highest)
        total = partial[:col_k]
        if sums is not None:
            sums = sum(g[1] for g in gathered)
            total = jnp.concatenate([total, sums])
        both = total
        for k in range(1, count_y):
            packed = partial[k * col_k : (k + 1) * col_k]
            if sums is not None:
                packed = jnp.concatenate([packed, sums])
            both = both + shifted(packed, "gy", -k)
        if split:
            both = lax.all_gather(both, "gz", axis=1, tiled=True)
        return both[:col_k], both[col_k:]

    def precondition(field, device_in, device_up, sums, extra):
        mine = device_up if sums is None else jnp.concatenate([device_up, sums])
        packed = lax.all_gather(mine, "gz", axis=0)
        column_in = packed[:, :rows_mine].reshape(-1, systems)
        chosen = column_in
        if sums is not None:
            sums = packed[:, rows_mine:].sum(0)
        if split:
            chosen = lax.dynamic_slice_in_dim(column_in, iz * part, part, 1)
            if sums is not None:
                sums = lax.dynamic_slice_in_dim(sums, iz * part, part, 1)
        column_up = lax.dot_general(col_v, chosen, (((0,), (0,)), ((), ())), precision=highest)
        top_out, sums = top_level(column_up, sums)
        leaf_near, dev_near, col_near = near(field, leaf_f, dev_f, device_in, col_f, column_in)
        if extra is not None:
            extra, sums = extra(sums)
        found = lift(
            top_out, col_w_mine, col_s, first_row.reshape(1), col_near,
            dev_w, dev_s, dev_near, leaf_w, leaf_s, leaf_near, extra or (),
        )
        return found, sums

    cond = conductivity.transpose(0, 2, 1)
    dims = (("gx", 0), ("gy", 2), ("gz", 1))
    diagonal = reaction.transpose(0, 2, 1)
    faces = []
    for axis, dim in dims:
        low = lax.index_in_dim(cond, 0, dim, keepdims=True)
        top = lax.index_in_dim(cond, cells - 1, dim, keepdims=True)
        below, above = exchange(low, top, axis)
        has_below = lax.axis_index(axis) > 0
        has_above = lax.axis_index(axis) < lax.axis_size(axis) - 1
        below = jnp.where(has_below, below, 0.0)
        above = jnp.where(has_above, above, 0.0)
        wide = jnp.concatenate([below, cond, above], axis=dim)
        face = 0.5 * (
            lax.slice_in_dim(wide, 0, cells + 1, axis=dim)
            + lax.slice_in_dim(wide, 1, cells + 2, axis=dim)
        )
        diagonal = diagonal + lax.slice_in_dim(face, 0, cells, axis=dim) + lax.slice_in_dim(face, 1, cells + 1, axis=dim)
        place = lax.broadcasted_iota(jnp.int32, face.shape, dim)
        closed = ((place == 0) & ~has_below) | ((place == cells) & ~has_above)
        faces.append(jnp.where(closed, 0.0, face))
    coefs = spread(
        faces[0], faces[1],
        lax.slice_in_dim(faces[2], 0, cells, axis=1),
        lax.slice_in_dim(faces[2], 1, cells + 1, axis=1),
        diagonal,
    )

    def summed(values):
        for axis in ("gz", "gy", "gx"):
            values = values + sum(shifted(values, axis, k) for k in range(1, lax.axis_size(axis)))
        return values

    device_in, device_up = restrict(right_side, leaf_w, leaf_s, dev_w, dev_s)
    found, _ = precondition(right_side, device_in, device_up, None, None)
    first, x_low, x_top, y_low, y_top, z_low, z_top = found
    halo = exchange(x_low, x_top, "gx") + exchange(y_low, y_top, "gy") + exchange(z_low, z_top, "gz")
    image, device_in, device_up, sums = operator(first, halo, coefs, right_side, leaf_w, leaf_s, dev_w, dev_s)

    def stepping(sums):
        step = sums[0:1] / sums[1:2]
        return (first, step), (sums[0:1], step)

    found, (energy, step) = precondition(image, device_in, device_up, sums, stepping)
    corrected, _, x_top, _, y_top, _, z_top = found
    halo = (from_below(x_top, "gx"), from_below(y_top, "gy"), from_below(z_top, "gz"))
    sums = summed(forms(corrected, halo, coefs, right_side, image, step))
    energy_new, curvature_new = sums[0:1], sums[1:2]
    mixing = energy_new / energy
    step_new = energy_new / (curvature_new - mixing * energy_new / step)
    return (step + step_new * mixing) * first + step_new * corrected


def solution(mesh):
    return jax.shard_map(
        local,
        mesh=mesh,
        in_specs=(
            P("gx", "gy", "gz", None),
            P("gx", "gy", "gz"),
            P("gx", "gy", "gz"),
            P("gx", "gy", "gz", None, None),
            P("gx", "gy", "gz", None, None),
            P("gx", "gy", "gz", None),
            P("gx", "gy", "gz", None, None),
            P("gx", "gy", "gz", None, None),
            P("gx", "gy", "gz", None),
            P("gx", "gy", "gz", None),
            P("gx", "gy", None, None),
            P("gx", "gy", None),
            P(("gx", "gy"), None),
        ),
        out_specs=P("gx", "gy", "gz", None),
        check_vma=False,
    )
```

```python
import functools

import jax
import jax.numpy as jnp
from jax import lax
from jax.experimental import pallas as pl
from jax.experimental.pallas import tpu as pltpu
from jax.sharding import PartitionSpec as P

BOX = 8
LANES = 128
MIB = 1 << 20
NEAR_SLOTS = 3
LOAD_MIB = 54

def halves(values):
    high = values.astype(jnp.bfloat16)
    return high, (values - high.astype(values.dtype)).astype(jnp.bfloat16)


def product(left, right, left_dim=1):
    left_high, left_low = left if isinstance(left, tuple) else halves(left)
    right_high, right_low = right if isinstance(right, tuple) else halves(right)

    def one(a, b):
        return lax.dot_general(
            a, b, (((left_dim,), (0,)), ((), ())), preferred_element_type=jnp.float32
        )

    return one(left_high, right_high) + (one(left_low, right_high) + one(left_high, right_low))


def folded(weight, skeleton, first=0):
    rows = lax.broadcasted_iota(jnp.int32, weight.shape, weight.ndim - 2) + first
    return weight + (rows == skeleton).astype(weight.dtype)


def folded_across(weight, skeleton):
    kept, rows = weight.shape
    shape = (kept, kept)
    diagonal = lax.broadcasted_iota(jnp.int32, shape, 0) == lax.broadcasted_iota(jnp.int32, shape, 1)
    spread_out = jnp.broadcast_to(skeleton.astype(jnp.float32), shape)
    place = jnp.where(diagonal, spread_out, 0.0).sum(1, keepdims=True)
    lane = lax.broadcasted_iota(jnp.int32, weight.shape, 1).astype(jnp.float32)
    return weight + (lane == place).astype(weight.dtype)


def box_place(index, per_side):
    return index // (per_side * per_side), index // per_side % per_side, index % per_side


def cost(flops, moved):
    return pl.CostEstimate(flops=flops, bytes_accessed=moved, transcendentals=0)


VMEM = pl.BlockSpec(memory_space=pltpu.VMEM)
SMEM = pl.BlockSpec(memory_space=pltpu.SMEM)
HBM = pl.BlockSpec(memory_space=pltpu.HBM)


def f32(*shape):
    return jax.ShapeDtypeStruct(shape, jnp.float32)


def limit(mib):
    return pltpu.CompilerParams(vmem_limit_bytes=mib * MIB)


def box_cells(box, per_side):
    return tuple(pl.ds(pl.multiple_of(p * BOX, BOX), BOX) for p in box_place(box, per_side))


def restrict_all(field, leaf_w, leaf_s, dev_w, dev_s, device_in, device_up):
    boxes, kept, _ = leaf_w.shape
    systems = field.shape[-1]
    per_side = field.shape[0] // BOX

    def one_box(box, carry):
        values = field[box_cells(box, per_side)].reshape(-1, systems)
        rows = pl.ds(pl.multiple_of(box * kept, kept), kept)
        device_in[rows] = product(folded_across(leaf_w[box], leaf_s[box]), values)
        return carry

    lax.fori_loop(0, boxes, one_box, 0, unroll=2)
    device_up[...] = product(folded(dev_w[...], dev_s[...]), device_in[...], 0)


def load_body(count_x, count_y, me, *refs):
    sources, refs = refs[:7], refs[7:]
    field, leaf_w, leaf_s, dev_w, dev_s, cond, device_in, up = refs[:8]
    blocks = refs[8 : 8 + count_y]
    top, sems = refs[8 + count_y :]
    cells = cond.shape[0]
    per_side = cells // BOX
    boxes, kept, _ = leaf_w.shape
    systems = field.shape[-1]
    rows = dev_w.shape[1]
    right, *rest = sources
    copies = []

    def bring(source, target):
        copy = pltpu.make_async_copy(source, target, sems.at[len(copies)])
        copy.start()
        copies.append(copy)
        return copy

    small = [bring(rest[0], leaf_w), bring(rest[1], leaf_s)]
    parts = []
    for a in range(per_side):
        for b in range(per_side):
            part = (slice(a * BOX, (a + 1) * BOX), slice(b * BOX, (b + 1) * BOX))
            parts.append((part, bring(right.at[part], field.at[part])))
    later = [bring(*pair) for pair in zip(rest[2:], (dev_w, dev_s, cond, top))]
    for copy in small:
        copy.wait()
    for index, (part, copy) in enumerate(parts):
        copy.wait()
        for c in range(per_side):
            box = index * per_side + c
            values = field[(*part, slice(c * BOX, (c + 1) * BOX))].reshape(-1, systems)
            device_in[box * kept : (box + 1) * kept] = product(
                folded_across(leaf_w[box], leaf_s[box]), values
            )
    for copy in later:
        copy.wait()
    up[:rows] = product(folded(dev_w[...], dev_s[...]), device_in[...], 0)
    put_faces(up, rows, *z_faces(cond))
    size = top.shape[0]
    for k, out in enumerate(blocks):
        column = lax.rem(me[1] + k, count_y)
        for p in range(count_x):
            lanes = pl.ds(pl.multiple_of((p * count_y + column) * size, size), size)
            out[p * size : (p + 1) * size] = top[:, lanes]
        put_faces(out, count_x * size, cond[:, 0], cond[:, cells - 1])


def load(me, right, leaf_w, leaf_s, dev_w, dev_s, cond, top, count_x, count_y):
    boxes, kept, _ = leaf_w.shape
    systems = right.shape[-1]
    cells = cond.shape[0]
    kept_arrays = (right, leaf_w, leaf_s, dev_w, dev_s, cond)
    size = top.shape[0]
    return pl.pallas_call(
        functools.partial(load_body, count_x, count_y),
        in_specs=[SMEM] + [HBM] * 7,
        out_specs=[VMEM] * (8 + count_y),
        out_shape=[jax.ShapeDtypeStruct(a.shape, a.dtype) for a in kept_arrays]
        + [f32(boxes * kept, systems), f32(dev_w.shape[1] + 2 * cells, systems)]
        + [f32(count_x * size + 2 * cells, size)] * count_y,
        scratch_shapes=[
            pltpu.VMEM(top.shape, jnp.float32),
            pltpu.SemaphoreType.DMA((6 + (cells // BOX) ** 2,)),
        ],
        compiler_params=limit(LOAD_MIB),
        cost_estimate=restrict_cost(right, leaf_w, dev_w),
        name="load",
    )(me, right, leaf_w, leaf_s, dev_w, dev_s, cond, top)


def z_faces(cond):
    cells = cond.shape[0]
    lane = lax.broadcasted_iota(jnp.int32, (cells, cells), 1)
    faces = []
    for place in (0, cells - 1):
        face = jnp.zeros((cells, cells), jnp.float32)
        for x in range(cells):
            chosen = jnp.broadcast_to(cond[x][:, place : place + 1], face.shape)
            face = jnp.where(lane == x, chosen, face)
        faces.append(face)
    return faces


def put_faces(ref, row, low, top):
    cells = low.shape[0]
    ref[row:] = jnp.zeros_like(ref[row:])
    ref[row : row + cells, :cells] = low
    ref[row + cells : row + 2 * cells, :cells] = top


def restrict_cost(field, leaf_w, dev_w):
    return cost(6 * field.shape[-1] * (leaf_w.size + dev_w.size), 4 * field.size)


def column_body(part, rows, first, me, packed, col_w, col_s, *rest):
    mine, column_in = rest[-2:]
    count, _, systems = packed.shape
    for k in range(count):
        column_in[k * rows : (k + 1) * rows] = packed[k, :rows]
    if part < systems:
        lanes = pl.ds(pl.multiple_of(me[2] * part, LANES), part)
    else:
        lanes = slice(None)
    size = col_w.shape[1]
    mine[:size] = product(folded(col_w[...], col_s[...]), column_in[:, lanes], 0)
    if first:
        cond = rest[0]
        put_faces(mine, size, cond[0], cond[cond.shape[0] - 1])
    else:
        mine[size:] = sum(packed[k, rows:, lanes] for k in range(count))


def column(part, rows, me, packed, col_w, col_s, cond):
    count, _, systems = packed.shape
    extra = () if cond is None else (cond,)
    tail = BOX if cond is None else 2 * cond.shape[0]
    return pl.pallas_call(
        functools.partial(column_body, part, rows, bool(extra)),
        in_specs=[SMEM] + [VMEM] * (3 + len(extra)),
        out_specs=[VMEM] * 2,
        out_shape=[f32(col_w.shape[1] + tail, part), f32(count * rows, systems)],
        compiler_params=limit(8),
        cost_estimate=cost(6 * part * col_w.size, 8 * packed.size),
        name="column",
    )(me, packed, col_w, col_s, *extra)


def top_body(count_x, count_y, summing, me, *refs):
    blocks = refs[:count_y]
    gathered = refs[count_y : count_y + count_x]
    outs = refs[count_y + count_x + 1 : -1]
    whole = refs[-1]
    size = blocks[0].shape[1]
    for k in range(count_x):
        place = lax.rem(me[0] + count_x - k, count_x)
        whole[pl.ds(pl.multiple_of(place * size, size), size)] = gathered[k][:size]
    right = halves(whole[...])
    for k in range(count_y):
        left = jnp.concatenate(
            [blocks[k][p * size : (p + 1) * size] for p in range(count_x)], axis=1
        )
        outs[k][:size] = product(left, right)
    if summing:
        total = sum(g[size:] for g in gathered)
        for k in range(count_y):
            outs[k][size:] = total


def top_level(me, blocks, gathered, after, summing):
    count_x, count_y = len(gathered), len(blocks)
    size = blocks[0].shape[1]
    part = gathered[0].shape[1]
    return pl.pallas_call(
        functools.partial(top_body, count_x, count_y, summing),
        in_specs=[SMEM] + [VMEM] * (count_y + count_x + 1),
        out_specs=[VMEM] * count_y,
        out_shape=[f32(size + BOX * summing, part)] * count_y,
        scratch_shapes=[pltpu.VMEM((count_x * size, part), jnp.float32)],
        compiler_params=limit(8),
        cost_estimate=cost(6 * part * count_x * count_y * size * size, 4 * count_x * count_y * size * size),
        name="top",
    )(me, *blocks, *gathered, after)


def near_body(first, count, has_into, wants_cat, field, leaf_f, *refs):
    refs = refs[has_into:]
    if wants_cat:
        dev_f, device_in, col_f, column_in, leaf_w, leaf_s = refs[:6]
        leaf_near, dev_near, col_near, cat, slots, sems = refs[6:]
    elif not has_into:
        dev_f, device_in, col_f, column_in, leaf_near, dev_near, col_near, slots, sems = refs
    else:
        leaf_near, slots, sems = refs
    systems = field.shape[-1]
    per_side = field.shape[0] // BOX

    def copy(box, slot):
        return pltpu.make_async_copy(leaf_f.at[box], slots.at[slot], sems.at[slot])

    for k in range(min(NEAR_SLOTS, count)):
        copy(first + k, k).start()
    if not has_into:
        dev_near[...] = product(dev_f[...], device_in[...])
        col_near[...] = product(col_f[...], column_in[...])

    def one_box(step, carry):
        box = first + step
        slot = lax.rem(step, NEAR_SLOTS)
        copy(box, slot).wait()
        here = box_cells(box, per_side)
        values = field[here].reshape(-1, systems)
        result = product(slots[slot], values)
        leaf_near[here] = result.reshape(BOX, BOX, BOX, systems)
        if wants_cat:
            high, low = halves(folded_across(leaf_w[box], leaf_s[box]).T)
            cat[box] = jnp.concatenate([high, low, high], axis=1)

        @pl.when(step + NEAR_SLOTS < count)
        def _():
            copy(box + NEAR_SLOTS, slot).start()

        return carry

    lax.fori_loop(0, count, one_box, 0)


def near(field, leaf_f, first, count, into=None, coarse=(), leaf=()):
    _, leaf_size, _ = leaf_f.shape
    systems = field.shape[-1]
    extra = coarse + leaf if into is None else (into,)
    out_shape = [f32(*field.shape)]
    flops = count * leaf_size * leaf_size
    if into is None:
        out_shape += [f32(coarse[0].shape[0], systems), f32(coarse[2].shape[0], systems)]
        flops += coarse[0].size + coarse[2].size
    if leaf:
        boxes, kept, _ = leaf[0].shape
        out_shape.append(jax.ShapeDtypeStruct((boxes, leaf_size, 3 * kept), jnp.bfloat16))
    return pl.pallas_call(
        functools.partial(near_body, first, count, into is not None, bool(leaf)),
        in_specs=[VMEM, HBM] + [VMEM] * len(extra),
        out_specs=[VMEM] * len(out_shape),
        out_shape=out_shape,
        scratch_shapes=[
            pltpu.VMEM((NEAR_SLOTS, leaf_size, leaf_size), jnp.float32),
            pltpu.SemaphoreType.DMA((NEAR_SLOTS,)),
        ],
        input_output_aliases={} if into is None else {2: 0},
        compiler_params=limit(12),
        cost_estimate=cost(6 * systems * flops, 4 * count * leaf_size * leaf_size),
        name="near",
    )(field, leaf_f, *extra)


def lift_body(unread, update, me, top_out, col_w, col_s, col_near, dev_w, dev_s, dev_near, cat, leaf_near, *rest):
    rest = rest[unread:]
    if update:
        base, step = rest[:2]
        rest = rest[2:]
    out, *sent, coarse = rest
    boxes = cat.shape[0]
    cells = out.shape[0]
    systems = out.shape[-1]
    per_side = cells // BOX
    count = col_near.shape[0]
    first = me[2] * count
    col_v = folded(col_w[pl.ds(pl.multiple_of(first, BOX), count)], col_s[...], first)
    column_out = col_near[...] + product(col_v, top_out[: col_w.shape[1]])
    device_out = dev_near[...] + product(folded(dev_w[...], dev_s[...]), column_out)
    coarse[...] = device_out.reshape(coarse.shape)
    odd = [0 if update else lax.rem(me[axis], 2) for axis in range(3)]

    def one_box(box, carry):
        places = box_place(box, per_side)
        here = box_cells(box, per_side)
        high, low = halves(coarse[box])
        far = jnp.dot(
            cat[box], jnp.concatenate([high, high, low]), preferred_element_type=jnp.float32
        )
        values = leaf_near[here] + far.reshape(BOX, BOX, BOX, systems)
        if update:
            values = base[here] - step[...] * values
        out[here] = values
        for axis in range(3):
            others = tuple(h for k, h in enumerate(here) if k != axis)
            for side, spot, at in ((0, 0, 0), (1, BOX - 1, per_side - 1)):
                for slot in (0, 1):
                    target = sent[2 * axis + slot]

                    def put(axis=axis, spot=spot, target=target, others=others):
                        target[others] = values[(slice(None),) * axis + (spot,)]

                    if update:
                        if slot == 1 - side:
                            pl.when(places[axis] == at)(put)
                    else:
                        wanted = odd[axis] == (1 - side if slot == 0 else side)
                        pl.when((places[axis] == at) & wanted)(put)
        return carry

    lax.fori_loop(0, boxes, one_box, 0, unroll=2)


def lift(me, top_out, col_w, col_s, col_near, dev_w, dev_s, dev_near, cat, leaf_near, unread, update):
    boxes, _, width = cat.shape
    systems = leaf_near.shape[-1]
    return pl.pallas_call(
        functools.partial(lift_body, len(unread), bool(update)),
        in_specs=[SMEM] + [VMEM] * (9 + len(unread) + len(update)),
        out_specs=[VMEM] * 7,
        out_shape=[f32(*leaf_near.shape)] + [f32(*leaf_near.shape[1:])] * 6,
        scratch_shapes=[pltpu.VMEM((boxes, width // 3, systems), jnp.float32)],
        compiler_params=limit(12),
        cost_estimate=cost(6 * systems * (cat.size // 3 + dev_w.size), 8 * leaf_near.size),
        name="lift",
    )(me, top_out, col_w, col_s, col_near, dev_w, dev_s, dev_near, cat, leaf_near, *unread, *update)


def spread(left):
    ones = jnp.ones((left.shape[1], LANES), jnp.bfloat16)
    total = None
    for _ in range(3):
        part = left.astype(jnp.bfloat16)
        left = left - part.astype(left.dtype)
        term = jnp.dot(part, ones, preferred_element_type=jnp.float32)
        total = term if total is None else total + term
    return total


def spread_rows(values):
    count, width = values.shape
    wanted = (count, width, LANES)
    shape = (count * width, width)
    repeated = jnp.concatenate(
        [jnp.broadcast_to(values[a : a + 1], (width, width)) for a in range(count)]
    )
    row = lax.rem(lax.broadcasted_iota(jnp.int32, shape, 0), width)
    lane = lax.broadcasted_iota(jnp.int32, shape, 1)
    return spread(jnp.where(row == lane, repeated, 0.0)).reshape(wanted)


def spread_columns(values):
    width, count = values.shape
    lane = lax.broadcasted_iota(jnp.int32, values.shape, 1)
    left = jnp.concatenate([jnp.where(lane == a, values, 0.0) for a in range(count)])
    return spread(left).reshape(count, width, LANES)


def coefs_body(counts, rows, me, cond, react, found, x_below, x_above, y_below, y_above, after, x_face, y_face, z_face, diag, xe, ye, ze, half):
    cells = cond.shape[0]
    col_k = x_below.shape[0] - 2 * cells
    top_rows = y_below.shape[0] - 2 * cells

    def fill(x, carry):
        half[x] = spread_rows(0.5 * cond[x])
        diag[x] = spread_rows(react[x])
        return carry

    lax.fori_loop(0, cells, fill, 0, unroll=4)
    place = lax.broadcasted_iota(jnp.int32, (cells, cells, LANES), 1)

    def faces(x, carry):
        here = half[x]
        along_y = here[:-1] + here[1:]
        along_z = jnp.where(place < cells - 1, here + pltpu.roll(here, cells - 1, 1), 0.0)
        y_face[x] = along_y
        z_face[x] = along_z
        nothing = jnp.zeros_like(here[:1])
        diag[x] = (
            diag[x]
            + along_z
            + pltpu.roll(along_z, 1, 1)
            + jnp.concatenate([along_y, nothing])
            + jnp.concatenate([nothing, along_y])
        )
        return carry

    lax.fori_loop(0, cells, faces, 0)

    def between(x, carry):
        face = half[x] + half[x + 1]
        x_face[x] = face
        diag[x] += face
        diag[x + 1] += face
        return carry

    lax.fori_loop(0, cells - 1, between, 0)

    below = jnp.maximum(me[2] - 1, 0)
    above = jnp.minimum(me[2] + 1, counts[2] - 1)
    last = cells - 1
    other = (
        (x_below[col_k + cells :, :cells], x_above[col_k : col_k + cells, :cells]),
        (y_below[top_rows + cells :, :cells], y_above[top_rows : top_rows + cells, :cells]),
        (
            found[below, rows + cells : rows + 2 * cells, :cells],
            found[above, rows : rows + cells, :cells],
        ),
    )
    own = ((cond[0], cond[last]), (cond[:, 0], cond[:, last]), z_faces(cond))
    for axis, edge in enumerate((xe, ye, ze)):
        for side, spot in ((0, 0), (1, last)):
            open_side = me[axis] > 0 if side == 0 else me[axis] < counts[axis] - 1
            mask = jnp.where(open_side, 1.0, 0.0).astype(jnp.float32)
            small = 0.5 * (own[axis][side] + mask * other[axis][side])
            face = spread_columns(small) if axis == 2 else spread_rows(small)
            edge[side] = mask * face
            if axis == 0:
                diag[spot] += face
            elif axis == 1:
                diag[:, spot] += face
            else:
                diag[:, :, spot] += face


def coefficients(counts, rows, me, cond, react, found, gathered, blocks, after):
    cells = cond.shape[0]
    ins = (me, cond, react, found, gathered[1], gathered[-1], blocks[1], blocks[-1], after)
    cube = f32(cells, cells, cells, LANES)
    edge = f32(2, cells, cells, LANES)
    return pl.pallas_call(
        functools.partial(coefs_body, counts, rows),
        in_specs=[SMEM] + [VMEM] * 8,
        out_specs=[VMEM] * 7,
        out_shape=[
            f32(cells - 1, cells, cells, LANES),
            f32(cells, cells - 1, cells, LANES),
            cube,
            cube,
            edge,
            edge,
            edge,
        ],
        scratch_shapes=[pltpu.VMEM(cube.shape, jnp.float32)],
        compiler_params=limit(12),
        cost_estimate=cost(4000 * cond.size * LANES, 16 * cond.size * LANES),
        name="coefs",
    )(*ins)


def wide(values, systems):
    return jnp.concatenate([values] * (systems // LANES), axis=-1)


def fold_rows(values):
    return values.reshape(-1, BOX, values.shape[-1]).sum(0)


def sweep_body(second, field, x_face, y_face, z_face, diagonal, right, *rest):
    if second:
        image, step, sums, parts = rest
    else:
        image, sums, parts = rest
    cells, _, depth, systems = field.shape
    parts[...] = jnp.zeros_like(parts)

    def plane(x, has_below, has_above):
        energy = parts[0]
        curvature = parts[1]
        for y in range(cells):
            here = field[x, y]
            total = wide(diagonal[x, y], systems) * here
            if has_below:
                total -= wide(x_face[x - 1, y], systems) * field[x - 1, y]
            if has_above:
                total -= wide(x_face[x, y], systems) * field[x + 1, y]
            if y > 0:
                total -= wide(y_face[x, y - 1], systems) * field[x, y - 1]
            if y < cells - 1:
                total -= wide(y_face[x, y], systems) * field[x, y + 1]
            face = wide(z_face[x, y], systems)
            total -= face * pltpu.roll(here, depth - 1, 0)
            total -= pltpu.roll(face * here, 1, 0)
            if second:
                energy += fold_rows((right[x, y] - step[...] * image[x, y]) * here)
            else:
                image[x, y] = total
                energy += fold_rows(right[x, y] * here)
            curvature += fold_rows(here * total)
        parts[0] = energy
        parts[1] = curvature

    def middle(x, carry):
        plane(x, True, True)
        return carry

    plane(0, False, True)
    lax.fori_loop(1, cells - 1, middle, 0)
    plane(cells - 1, True, False)
    sums[...] = jnp.concatenate(
        [
            parts[0].sum(0, keepdims=True),
            parts[1].sum(0, keepdims=True),
            jnp.zeros((BOX - 2, systems), jnp.float32),
        ]
    )


def sweep(field, coefs, right, extra=()):
    systems = field.shape[-1]
    ins = (field, *coefs, right, *extra)
    outs = [f32(BOX, systems)]
    if not extra:
        outs = [f32(*field.shape)] + outs
    return pl.pallas_call(
        functools.partial(sweep_body, bool(extra)),
        in_specs=[VMEM] * len(ins),
        out_specs=[VMEM] * len(outs),
        out_shape=outs,
        scratch_shapes=[pltpu.VMEM((2, BOX, systems), jnp.float32)],
        compiler_params=limit(8),
        cost_estimate=cost(2000 * field.size, 16 * field.size),
        name="sweep",
    )(*ins)


def border_body(sizes, me, image_in, sums_in, xe, ye, ze, *rest):
    pairs = []
    for size in sizes:
        pairs.append([(rest[2 * k], rest[2 * k + 1]) for k in range(size)])
        rest = rest[2 * size :]
    leaf_w, leaf_s, dev_w, dev_s, image, device_in, up = rest
    cells, _, depth, systems = image.shape
    odd = [lax.rem(me[axis], 2) for axis in range(3)]

    def along(a, total):
        for axis, edge in ((0, xe), (1, ye)):
            for k, (own, halo) in enumerate(pairs[axis]):
                side = odd[axis] if k else 1 - odd[axis]
                spot = side * (cells - 1)
                term = wide(edge[side, a], systems) * halo[a]
                if axis == 0:
                    image[spot, a] -= term
                else:
                    image[a, spot] -= term
                total += own[a] * term
        for k, (own, halo) in enumerate(pairs[2]):
            side = odd[2] if k else 1 - odd[2]
            for here, spot in ((0, 0), (1, depth - 1)):
                chosen = jnp.where(side == here, 1.0, 0.0).astype(jnp.float32)
                term = wide(chosen * ze[here, a], systems) * halo[a]
                image[a, :, spot] -= term
                total += own[a] * term
        return total

    total = lax.fori_loop(0, cells, along, jnp.zeros((cells, systems), jnp.float32))
    rows = dev_w.shape[1]
    up[rows:] = sums_in[...]
    up[rows + 1 : rows + 2] = sums_in[1:2] - total.sum(0, keepdims=True)
    restrict_all(image, leaf_w, leaf_s, dev_w, dev_s, device_in, up.at[:rows])


def border(me, image, sums, edges, pairs, leaf_w, leaf_s, dev_w, dev_s):
    boxes, kept, _ = leaf_w.shape
    systems = image.shape[-1]
    flat = [array for found in pairs for pair in found for array in pair]
    ins = (me, image, sums, *edges, *flat, leaf_w, leaf_s, dev_w, dev_s)
    return pl.pallas_call(
        functools.partial(border_body, [len(found) for found in pairs]),
        in_specs=[SMEM] + [VMEM] * (len(ins) - 1),
        out_specs=[VMEM] * 3,
        out_shape=[
            f32(*image.shape),
            f32(boxes * kept, systems),
            f32(dev_w.shape[1] + BOX, systems),
        ],
        input_output_aliases={1: 0},
        compiler_params=limit(12),
        cost_estimate=restrict_cost(image, leaf_w, dev_w),
        name="border",
    )(*ins)


def across_body(sums_in, xe, ye, ze, x_own, y_own, z_own, x_halo, y_halo, z_halo, sums):
    cells, _, systems = x_halo.shape

    def along(a, total):
        total += wide(xe[0, a], systems) * x_own[a] * x_halo[a]
        total += wide(ye[0, a], systems) * y_own[a] * y_halo[a]
        return total + wide(ze[0, a], systems) * z_own[a] * z_halo[a]

    total = lax.fori_loop(0, cells, along, jnp.zeros((cells, systems), jnp.float32))
    sums[...] = sums_in[...]
    sums[1:2] = sums_in[1:2] - 2.0 * total.sum(0, keepdims=True)


def across(sums, edges, own, halo):
    ins = (sums, *edges, *own, *halo)
    return pl.pallas_call(
        across_body,
        in_specs=[VMEM] * len(ins),
        out_specs=VMEM,
        out_shape=f32(*sums.shape),
        compiler_params=limit(8),
        cost_estimate=cost(own[0].size * 20, own[0].size * 24),
        name="across",
    )(*ins)


def shifted(values, axis, step):
    count = lax.axis_size(axis)
    return lax.ppermute(values, axis, [(i, (i + step) % count) for i in range(count)])


def mirrored(sent, axis):
    count = lax.axis_size(axis)
    found = []
    for start in (0, 1) if count > 2 else (0,):
        pairs = []
        for i in range(count):
            j = ((i - start) ^ 1) + start
            pairs.append((i, j if 0 <= j < count else i))
        found.append((sent[start], lax.ppermute(sent[start], axis, pairs)))
    return found


def finish_body(first, corrected, sums, energy, step, out):
    energy_new, curvature_new = sums[0:1], sums[1:2]
    mixing = energy_new / energy[...]
    step_new = energy_new / (curvature_new - mixing * energy_new / step[...])
    out[...] = (step[...] + step_new * mixing) * first[...] + step_new * corrected[...]


def finish(first, corrected, sums, energy, step):
    cells = first.shape[0]
    plane = pl.BlockSpec((2, *first.shape[1:]), lambda i: (i, 0, 0, 0))

    def whole(array):
        return pl.BlockSpec(array.shape, lambda i: (0, 0))

    return pl.pallas_call(
        finish_body,
        grid=(cells // 2,),
        in_specs=[plane, plane, whole(sums), whole(energy), whole(step)],
        out_specs=plane,
        out_shape=f32(*first.shape),
        compiler_params=limit(8),
        name="finish",
    )(first, corrected, sums, energy, step)


def local(
    right_side,
    conductivity,
    reaction,
    leaf_factor,
    leaf_weight,
    leaf_skeleton,
    device_factor,
    device_weight,
    device_skeleton,
    column_factor,
    column_weight,
    column_skeleton,
    top_factor,
):
    cells = right_side.shape[0]
    systems = right_side.shape[3]
    boxes = (cells // BOX) ** 3
    leaf_size = BOX**3
    count_x, count_y, count_z = (lax.axis_size(a) for a in ("gx", "gy", "gz"))
    ix, iy, iz = (lax.axis_index(a) for a in ("gx", "gy", "gz"))
    leaf_f = leaf_factor.reshape(boxes, leaf_size, leaf_size)
    dev_f = device_factor[0, 0, 0]
    col_f = column_factor[0, 0]
    col_w = column_weight[0, 0]
    col_s = column_skeleton[0]
    dev_s = device_skeleton[0, 0]
    me = jnp.stack([ix, iy, iz])
    right_side, leaf_w, leaf_s, dev_w, dev_s, conductivity, device_in, device_up, *packed = load(
        me,
        right_side,
        jnp.swapaxes(leaf_weight, -1, -2).reshape(boxes, -1, leaf_size),
        leaf_skeleton.reshape(boxes, 1, -1),
        device_weight[0, 0, 0],
        dev_s,
        conductivity,
        top_factor,
        count_x,
        count_y,
    )
    levels = (leaf_w, leaf_s, dev_w, dev_s)
    rows_mine = dev_w.shape[1]
    col_k = col_w.shape[1]
    part = systems // count_z
    if part % LANES:
        part = systems

    blocks = [packed[0]] + [shifted(packed[k], "gy", k) for k in range(1, count_y)]

    def precondition(field, device_in, device_up, cond, cat, between):
        found = lax.all_gather(device_up, "gz", axis=0)
        mine, column_in = column(part, rows_mine, me, found, col_w, col_s, cond)
        gathered = [mine] + [shifted(mine, "gx", k) for k in range(1, count_x)]
        coarse = (dev_f, device_in, col_f, column_in)
        if cat is None:
            leaf_near, dev_near, col_near, cat = near(
                field, leaf_f, 0, boxes, coarse=coarse, leaf=(leaf_w, leaf_s)
            )
        else:
            part_near, dev_near, col_near = near(field, leaf_f, 0, boxes // 2, coarse=coarse)
            (leaf_near,) = near(field, leaf_f, boxes // 2, boxes // 2, into=part_near)
        partial = top_level(me, blocks, gathered, dev_near, cond is None)
        total = partial[0]
        for k in range(1, count_y):
            total = total + shifted(partial[k], "gy", -k)
        if part < systems:
            total = lax.all_gather(total, "gz", axis=1, tiled=True)
        extra, kept = between(found, gathered, total, partial[1])
        lifted = lift(
            me, total, col_w, col_s, col_near,
            dev_w, dev_s, dev_near, cat, leaf_near, *extra,
        )
        return lifted, (kept, cat)

    def first_between(found, gathered, total, partial):
        counts = (count_x, count_y, count_z)
        out = coefficients(counts, rows_mine, me, conductivity, reaction, found, gathered, blocks, partial)
        return ((out[3],), ()), (out[:4], out[4:])

    def second_between(found, gathered, total, partial):
        sums = total[col_k:]
        step = sums[0:1] / sums[1:2]
        return ((), (first, step)), (sums[0:1], step)

    def summed(values):
        for axis in ("gz", "gy", "gx"):
            values = values + sum(shifted(values, axis, k) for k in range(1, lax.axis_size(axis)))
        return values

    lifted, ((coefs, edges), cat) = precondition(
        right_side, device_in, device_up, conductivity, None, first_between
    )
    first, own = lifted[0], lifted[1:]
    pairs = [mirrored(own[2 * k : 2 * k + 2], axis) for k, axis in enumerate(("gx", "gy", "gz"))]
    image, sums = sweep(first, coefs, right_side)
    image, device_in, device_up = border(me, image, sums, edges, pairs, *levels)

    lifted, ((energy, step), _) = precondition(image, device_in, device_up, None, cat, second_between)
    corrected, own = lifted[0], lifted[1:]
    halo = [shifted(top, axis, 1) for top, axis in zip(own[::2], ("gx", "gy", "gz"))]
    (sums,) = sweep(corrected, coefs, right_side, (image, step))
    sums = summed(across(sums, edges, own[1::2], halo))
    return finish(first, corrected, sums, energy, step)


def solution(mesh):
    return jax.shard_map(
        local,
        mesh=mesh,
        in_specs=(
            P("gx", "gy", "gz", None),
            P("gx", "gy", "gz"),
            P("gx", "gy", "gz"),
            P("gx", "gy", "gz", None, None),
            P("gx", "gy", "gz", None, None),
            P("gx", "gy", "gz", None),
            P("gx", "gy", "gz", None, None),
            P("gx", "gy", "gz", None, None),
            P("gx", "gy", "gz", None),
            P("gx", "gy", "gz", None),
            P("gx", "gy", None, None),
            P("gx", "gy", None),
            P(("gx", "gy"), None),
        ),
        out_specs=P("gx", "gy", "gz", None),
        check_vma=False,
    )
```

```python
import functools

import jax
import jax.numpy as jnp
from jax import lax
from jax.experimental import pallas as pl
from jax.experimental.pallas import tpu as pltpu
from jax.sharding import PartitionSpec as P

BOX = 8
LANES = 128
MIB = 1 << 20
NEAR_SLOTS = 3
LOAD_MIB = 16

def halves(values):
    high = values.astype(jnp.bfloat16)
    return high, (values - high.astype(values.dtype)).astype(jnp.bfloat16)


def product(left, right, left_dim=1):
    left_high, left_low = left if isinstance(left, tuple) else halves(left)
    right_high, right_low = right if isinstance(right, tuple) else halves(right)

    def one(a, b):
        return lax.dot_general(
            a, b, (((left_dim,), (0,)), ((), ())), preferred_element_type=jnp.float32
        )

    rows = left_high.shape[1 - left_dim]
    both = one(jnp.concatenate([left_high, left_low], axis=1 - left_dim), right_high)
    return both[:rows] + (both[rows:] + one(left_high, right_low))


def folded(weight, skeleton, first=0):
    rows = lax.broadcasted_iota(jnp.int32, weight.shape, weight.ndim - 2) + first
    return weight + (rows == skeleton).astype(weight.dtype)


def folded_across(weight, skeleton):
    kept, rows = weight.shape
    shape = (kept, kept)
    diagonal = lax.broadcasted_iota(jnp.int32, shape, 0) == lax.broadcasted_iota(jnp.int32, shape, 1)
    spread_out = jnp.broadcast_to(skeleton.astype(jnp.float32), shape)
    place = jnp.where(diagonal, spread_out, 0.0).sum(1, keepdims=True)
    lane = lax.broadcasted_iota(jnp.int32, weight.shape, 1).astype(jnp.float32)
    return weight + (lane == place).astype(weight.dtype)


def box_place(index, per_side):
    return index // (per_side * per_side), index // per_side % per_side, index % per_side


def cost(flops, moved):
    return pl.CostEstimate(flops=flops, bytes_accessed=moved, transcendentals=0)


VMEM = pl.BlockSpec(memory_space=pltpu.VMEM)
HBM = pl.BlockSpec(memory_space=pltpu.HBM)


def f32(*shape):
    return jax.ShapeDtypeStruct(shape, jnp.float32)


def position():
    return tuple(lax.axis_index(axis) for axis in ("gx", "gy", "gz"))


def limit(mib):
    return pltpu.CompilerParams(vmem_limit_bytes=mib * MIB)


def box_cells(box, per_side):
    return tuple(pl.ds(pl.multiple_of(p * BOX, BOX), BOX) for p in box_place(box, per_side))


def restrict_all(field, leaf_w, leaf_s, dev_w, dev_s, device_in, device_up):
    boxes, kept, _ = leaf_w.shape
    systems = field.shape[-1]
    per_side = field.shape[0] // BOX

    def one_box(box, carry):
        values = field[box_cells(box, per_side)].reshape(-1, systems)
        rows = pl.ds(pl.multiple_of(box * kept, kept), kept)
        device_in[rows] = product(folded_across(leaf_w[box], leaf_s[box]), values)
        return carry

    lax.fori_loop(0, boxes, one_box, 0, unroll=2)
    device_up[...] = product(folded(dev_w[...], dev_s[...]), device_in[...], 0)


def load_body(count_x, count_y, *refs):
    me = position()
    sources, refs = refs[:12], refs[12:]
    field, leaf_w, leaf_s, dev_w, dev_s, cond, *others, device_in, up = refs[:13]
    blocks = refs[13 : 13 + count_y]
    top, sems = refs[13 + count_y :]
    cells = cond.shape[0]
    per_side = cells // BOX
    boxes, kept, _ = leaf_w.shape
    systems = field.shape[-1]
    rows = dev_w.shape[1]
    right, *rest = sources
    copies = []

    def bring(source, target):
        copy = pltpu.make_async_copy(source, target, sems.at[len(copies)])
        copy.start()
        copies.append(copy)
        return copy

    small = [bring(rest[0], leaf_w), bring(rest[1], leaf_s)]
    parts = []
    for a in range(per_side):
        for b in range(per_side):
            parts.append((slice(a * BOX, (a + 1) * BOX), slice(b * BOX, (b + 1) * BOX)))
    ahead = 2
    waits = [bring(right.at[part], field.at[part]) for part in parts[:ahead]]
    later = []
    for copy in small:
        copy.wait()
    for index, part in enumerate(parts):
        waits[index].wait()
        if index + ahead < len(parts):
            part_ahead = parts[index + ahead]
            waits.append(bring(right.at[part_ahead], field.at[part_ahead]))
        elif not later:
            later = [bring(*pair) for pair in zip(rest[2:], (dev_w, dev_s, cond, top, *others))]
        for c in range(per_side):
            box = index * per_side + c
            values = field[(*part, slice(c * BOX, (c + 1) * BOX))].reshape(-1, systems)
            device_in[box * kept : (box + 1) * kept] = product(
                folded_across(leaf_w[box], leaf_s[box]), values
            )
    for copy in later:
        copy.wait()
    up[:rows] = product(folded(dev_w[...], dev_s[...]), device_in[...], 0)
    put_faces(up, rows, *z_faces(cond))
    size = top.shape[0]
    for k, out in enumerate(blocks):
        column = lax.rem(me[1] + k, count_y)
        for p in range(count_x):
            lanes = pl.ds(pl.multiple_of((p * count_y + column) * size, size), size)
            out[p * size : (p + 1) * size] = top[:, lanes]
        put_faces(out, count_x * size, cond[:, 0], cond[:, cells - 1])


def load(right, leaf_w, leaf_s, dev_w, dev_s, cond, top, others, count_x, count_y):
    boxes, kept, _ = leaf_w.shape
    systems = right.shape[-1]
    cells = cond.shape[0]
    kept_arrays = (right, leaf_w, leaf_s, dev_w, dev_s, cond, *others)
    size = top.shape[0]
    return pl.pallas_call(
        functools.partial(load_body, count_x, count_y),
        in_specs=[HBM] * 12,
        out_specs=[VMEM] * (13 + count_y),
        out_shape=[jax.ShapeDtypeStruct(a.shape, a.dtype) for a in kept_arrays]
        + [f32(boxes * kept, systems), f32(dev_w.shape[1] + 2 * cells, systems)]
        + [f32(count_x * size + 2 * cells, size)] * count_y,
        scratch_shapes=[
            pltpu.VMEM(top.shape, jnp.float32),
            pltpu.SemaphoreType.DMA((11 + (cells // BOX) ** 2,)),
        ],
        compiler_params=limit(LOAD_MIB),
        cost_estimate=restrict_cost(right, leaf_w, dev_w),
        name="load",
    )(*(pltpu.with_memory_space_constraint(a, pltpu.HBM) for a in (right, leaf_w, leaf_s, dev_w, dev_s, cond, top, *others)))


def z_faces(cond):
    cells = cond.shape[0]
    lane = lax.broadcasted_iota(jnp.int32, (cells, cells), 1)
    faces = []
    for place in (0, cells - 1):
        face = jnp.zeros((cells, cells), jnp.float32)
        for x in range(cells):
            chosen = jnp.broadcast_to(cond[x][:, place : place + 1], face.shape)
            face = jnp.where(lane == x, chosen, face)
        faces.append(face)
    return faces


def put_faces(ref, row, low, top):
    cells = low.shape[0]
    ref[row:] = jnp.zeros_like(ref[row:])
    ref[row : row + cells, :cells] = low
    ref[row + cells : row + 2 * cells, :cells] = top


def restrict_cost(field, leaf_w, dev_w):
    return cost(6 * field.shape[-1] * (leaf_w.size + dev_w.size), 4 * field.size)


def column_body(part, rows, first, count, *refs):
    me = position()
    found = refs[:count]
    col_w, col_s = refs[count : count + 2]
    mine, column_in = refs[-2:]
    systems = column_in.shape[1]
    for k in range(count):
        place = lax.rem(me[2] + count - k, count)
        column_in[pl.ds(pl.multiple_of(place * rows, BOX), rows)] = found[k][:rows]
    if part < systems:
        lanes = pl.ds(pl.multiple_of(me[2] * part, LANES), part)
    else:
        lanes = slice(None)
    size = col_w.shape[1]
    mine[:size] = product(folded(col_w[...], col_s[...]), column_in[:, lanes], 0)
    if first:
        cond = refs[count + 2]
        put_faces(mine, size, cond[0], cond[cond.shape[0] - 1])
    else:
        mine[size:] = sum(f[rows:, lanes] for f in found)


def column(part, rows, found, col_w, col_s, cond):
    count = len(found)
    systems = found[0].shape[1]
    extra = () if cond is None else (cond,)
    tail = BOX if cond is None else 2 * cond.shape[0]
    return pl.pallas_call(
        functools.partial(column_body, part, rows, bool(extra), count),
        in_specs=[VMEM] * (count + 2 + len(extra)),
        out_specs=[VMEM] * 2,
        out_shape=[f32(col_w.shape[1] + tail, part), f32(count * rows, systems)],
        compiler_params=limit(8),
        cost_estimate=cost(6 * part * col_w.size, 8 * count * rows * systems),
        name="column",
    )(*found, col_w, col_s, *extra)


def top_body(count_x, count_y, summing, *refs):
    me = position()
    blocks = refs[:count_y]
    gathered = refs[count_y : count_y + count_x]
    outs = refs[count_y + count_x + 1 : -1]
    whole = refs[-1]
    size = blocks[0].shape[1]
    for k in range(count_x):
        place = lax.rem(me[0] + count_x - k, count_x)
        whole[pl.ds(pl.multiple_of(place * size, size), size)] = gathered[k][:size]
    right = halves(whole[...])
    for k in range(count_y):
        left = jnp.concatenate(
            [blocks[k][p * size : (p + 1) * size] for p in range(count_x)], axis=1
        )
        outs[k][:size] = product(left, right)
    if summing:
        total = sum(g[size:] for g in gathered)
        for k in range(count_y):
            outs[k][size:] = total


def top_level(blocks, gathered, after, summing):
    count_x, count_y = len(gathered), len(blocks)
    size = blocks[0].shape[1]
    part = gathered[0].shape[1]
    return pl.pallas_call(
        functools.partial(top_body, count_x, count_y, summing),
        in_specs=[VMEM] * (count_y + count_x + 1),
        out_specs=[VMEM] * count_y,
        out_shape=[f32(size + BOX * summing, part)] * count_y,
        scratch_shapes=[pltpu.VMEM((count_x * size, part), jnp.float32)],
        compiler_params=limit(8),
        cost_estimate=cost(6 * part * count_x * count_y * size * size, 4 * count_x * count_y * size * size),
        name="top",
    )(*blocks, *gathered, after)


def near_body(first, count, has_into, wants_cat, field, leaf_f, *refs):
    refs = refs[has_into:]
    if wants_cat:
        dev_f, device_in, col_f, column_in, leaf_w, leaf_s = refs[:6]
        leaf_near, dev_near, col_near, cat, slots, sems = refs[6:]
    elif not has_into:
        dev_f, device_in, col_f, column_in, leaf_near, dev_near, col_near, slots, sems = refs
    else:
        leaf_near, slots, sems = refs
    systems = field.shape[-1]
    per_side = field.shape[0] // BOX

    def copy(box, slot):
        return pltpu.make_async_copy(leaf_f.at[box], slots.at[slot], sems.at[slot])

    for k in range(min(NEAR_SLOTS, count)):
        copy(first + k, k).start()
    if not has_into:
        dev_near[...] = product(dev_f[...], device_in[...])
        col_near[...] = product(col_f[...], column_in[...])

    def one_box(step, carry):
        box = first + step
        slot = lax.rem(step, NEAR_SLOTS)
        copy(box, slot).wait()
        here = box_cells(box, per_side)
        values = field[here].reshape(-1, systems)
        result = product(slots[slot], values)
        leaf_near[here] = result.reshape(BOX, BOX, BOX, systems)
        if wants_cat:
            high, low = halves(folded_across(leaf_w[box], leaf_s[box]).T)
            cat[box] = jnp.concatenate([high, low, high], axis=1)

        @pl.when(step + NEAR_SLOTS < count)
        def _():
            copy(box + NEAR_SLOTS, slot).start()

        return carry

    lax.fori_loop(0, count, one_box, 0)


def near(field, leaf_f, first, count, into=None, coarse=(), leaf=()):
    _, leaf_size, _ = leaf_f.shape
    systems = field.shape[-1]
    extra = coarse + leaf if into is None else (into,)
    out_shape = [f32(*field.shape)]
    flops = count * leaf_size * leaf_size
    if into is None:
        out_shape += [f32(coarse[0].shape[0], systems), f32(coarse[2].shape[0], systems)]
        flops += coarse[0].size + coarse[2].size
    if leaf:
        boxes, kept, _ = leaf[0].shape
        out_shape.append(jax.ShapeDtypeStruct((boxes, leaf_size, 3 * kept), jnp.bfloat16))
    return pl.pallas_call(
        functools.partial(near_body, first, count, into is not None, bool(leaf)),
        in_specs=[VMEM, HBM] + [VMEM] * len(extra),
        out_specs=[VMEM] * len(out_shape),
        out_shape=out_shape,
        scratch_shapes=[
            pltpu.VMEM((NEAR_SLOTS, leaf_size, leaf_size), jnp.float32),
            pltpu.SemaphoreType.DMA((NEAR_SLOTS,)),
        ],
        input_output_aliases={} if into is None else {2: 0},
        compiler_params=limit(12),
        cost_estimate=cost(6 * systems * flops, 4 * count * leaf_size * leaf_size),
        name="near",
    )(field, leaf_f, *extra)


def lift_body(unread, update, count_z, *refs):
    me = position()
    parts, refs = refs[:count_z], refs[count_z:]
    col_w, col_s, col_near, dev_w, dev_s, dev_near, cat, leaf_near, *rest = refs
    rest = rest[unread:]
    if update:
        base, rest = rest[0], rest[1:]
        kept, coarse, top_out = rest[7:]
    else:
        coarse, top_out = rest[7:]
    out, *sent = rest[:7]
    size = col_w.shape[1]
    part = parts[0].shape[1]
    for k in range(count_z):
        lanes = lax.rem(me[2] + count_z - k, count_z) * part
        top_out[:, pl.ds(pl.multiple_of(lanes, LANES), part)] = parts[k][...]
    if update:
        energy = top_out[size : size + 1]
        step = energy / top_out[size + 1 : size + 2]
        kept[...] = jnp.zeros_like(kept)
        kept[0:1] = energy
        kept[1:2] = step
    boxes = cat.shape[0]
    cells = out.shape[0]
    systems = out.shape[-1]
    per_side = cells // BOX
    count = col_near.shape[0]
    first = me[2] * count
    col_v = folded(col_w[pl.ds(pl.multiple_of(first, BOX), count)], col_s[...], first)
    column_out = col_near[...] + product(col_v, top_out[:size])
    device_out = dev_near[...] + product(folded(dev_w[...], dev_s[...]), column_out)
    coarse[...] = device_out.reshape(coarse.shape)
    odd = [0 if update else lax.rem(me[axis], 2) for axis in range(3)]

    def one_box(box, carry):
        places = box_place(box, per_side)
        here = box_cells(box, per_side)
        high, low = halves(coarse[box])
        far = jnp.dot(
            cat[box], jnp.concatenate([high, high, low]), preferred_element_type=jnp.float32
        )
        values = leaf_near[here] + far.reshape(BOX, BOX, BOX, systems)
        if update:
            values = base[here] - step * values
        out[here] = values
        for axis in range(3):
            others = tuple(h for k, h in enumerate(here) if k != axis)
            for side, spot, at in ((0, 0, 0), (1, BOX - 1, per_side - 1)):
                for slot in (0, 1):
                    target = sent[2 * axis + slot]

                    def put(axis=axis, spot=spot, target=target, others=others):
                        target[others] = values[(slice(None),) * axis + (spot,)]

                    if update:
                        if slot == 1 - side:
                            pl.when(places[axis] == at)(put)
                    else:
                        wanted = odd[axis] == (1 - side if slot == 0 else side)
                        pl.when((places[axis] == at) & wanted)(put)
        return carry

    lax.fori_loop(0, boxes, one_box, 0, unroll=2)


def lift(parts, col_w, col_s, col_near, dev_w, dev_s, dev_near, cat, leaf_near, unread, update):
    boxes, _, width = cat.shape
    systems = leaf_near.shape[-1]
    out_shape = [f32(*leaf_near.shape)] + [f32(*leaf_near.shape[1:])] * 6
    if update:
        out_shape.append(f32(BOX, systems))
    return pl.pallas_call(
        functools.partial(lift_body, len(unread), bool(update), len(parts)),
        in_specs=[VMEM] * (len(parts) + 8 + len(unread) + len(update)),
        out_specs=[VMEM] * len(out_shape),
        out_shape=out_shape,
        scratch_shapes=[
            pltpu.VMEM((boxes, width // 3, systems), jnp.float32),
            pltpu.VMEM((parts[0].shape[0], systems), jnp.float32),
        ],
        compiler_params=limit(12),
        cost_estimate=cost(6 * systems * (cat.size // 3 + dev_w.size), 8 * leaf_near.size),
        name="lift",
    )(*parts, col_w, col_s, col_near, dev_w, dev_s, dev_near, cat, leaf_near, *unread, *update)


def spread(left):
    ones = jnp.ones((left.shape[1], LANES), jnp.bfloat16)
    total = None
    for _ in range(3):
        part = left.astype(jnp.bfloat16)
        left = left - part.astype(left.dtype)
        term = jnp.dot(part, ones, preferred_element_type=jnp.float32)
        total = term if total is None else total + term
    return total


def spread_rows(values):
    count, width = values.shape
    wanted = (count, width, LANES)
    shape = (count * width, width)
    repeated = jnp.concatenate(
        [jnp.broadcast_to(values[a : a + 1], (width, width)) for a in range(count)]
    )
    row = lax.rem(lax.broadcasted_iota(jnp.int32, shape, 0), width)
    lane = lax.broadcasted_iota(jnp.int32, shape, 1)
    return spread(jnp.where(row == lane, repeated, 0.0)).reshape(wanted)


def spread_columns(values):
    width, count = values.shape
    lane = lax.broadcasted_iota(jnp.int32, values.shape, 1)
    left = jnp.concatenate([jnp.where(lane == a, values, 0.0) for a in range(count)])
    return spread(left).reshape(count, width, LANES)


def coefs_body(counts, rows, cond, react, z_below, z_above, x_below, x_above, y_below, y_above, after, x_face, y_face, z_face, diag, xe, ye, ze, half):
    me = position()
    cells = cond.shape[0]
    col_k = x_below.shape[0] - 2 * cells
    top_rows = y_below.shape[0] - 2 * cells

    def fill(x, carry):
        half[x] = spread_rows(0.5 * cond[x])
        diag[x] = spread_rows(react[x])
        return carry

    lax.fori_loop(0, cells, fill, 0, unroll=4)
    place = lax.broadcasted_iota(jnp.int32, (cells, cells, LANES), 1)

    def faces(x, carry):
        here = half[x]
        along_y = here[:-1] + here[1:]
        along_z = jnp.where(place < cells - 1, here + pltpu.roll(here, cells - 1, 1), 0.0)
        y_face[x] = along_y
        z_face[x] = along_z
        nothing = jnp.zeros_like(here[:1])
        diag[x] = (
            diag[x]
            + along_z
            + pltpu.roll(along_z, 1, 1)
            + jnp.concatenate([along_y, nothing])
            + jnp.concatenate([nothing, along_y])
        )
        return carry

    lax.fori_loop(0, cells, faces, 0)

    def between(x, carry):
        face = half[x] + half[x + 1]
        x_face[x] = face
        diag[x] += face
        diag[x + 1] += face
        return carry

    lax.fori_loop(0, cells - 1, between, 0)

    last = cells - 1
    other = (
        (x_below[col_k + cells :, :cells], x_above[col_k : col_k + cells, :cells]),
        (y_below[top_rows + cells :, :cells], y_above[top_rows : top_rows + cells, :cells]),
        (z_below[rows + cells :, :cells], z_above[rows : rows + cells, :cells]),
    )
    own = ((cond[0], cond[last]), (cond[:, 0], cond[:, last]), z_faces(cond))
    for axis, edge in enumerate((xe, ye, ze)):
        for side, spot in ((0, 0), (1, last)):
            open_side = me[axis] > 0 if side == 0 else me[axis] < counts[axis] - 1
            mask = jnp.where(open_side, 1.0, 0.0).astype(jnp.float32)
            small = 0.5 * (own[axis][side] + mask * other[axis][side])
            face = spread_columns(small) if axis == 2 else spread_rows(small)
            edge[side] = mask * face
            if axis == 0:
                diag[spot] += face
            elif axis == 1:
                diag[:, spot] += face
            else:
                diag[:, :, spot] += face


def coefficients(counts, rows, cond, react, found, gathered, blocks, after):
    cells = cond.shape[0]
    ins = (cond, react, found[1], found[-1], gathered[1], gathered[-1], blocks[1], blocks[-1], after)
    cube = f32(cells, cells, cells, LANES)
    edge = f32(2, cells, cells, LANES)
    return pl.pallas_call(
        functools.partial(coefs_body, counts, rows),
        in_specs=[VMEM] * 9,
        out_specs=[VMEM] * 7,
        out_shape=[
            f32(cells - 1, cells, cells, LANES),
            f32(cells, cells - 1, cells, LANES),
            cube,
            cube,
            edge,
            edge,
            edge,
        ],
        scratch_shapes=[pltpu.VMEM(cube.shape, jnp.float32)],
        compiler_params=limit(12),
        cost_estimate=cost(4000 * cond.size * LANES, 16 * cond.size * LANES),
        name="coefs",
    )(*ins)


def wide(values, systems):
    return jnp.concatenate([values] * (systems // LANES), axis=-1)


def fold_rows(values):
    return values.reshape(-1, BOX, values.shape[-1]).sum(0)


def sweep_body(second, field, x_face, y_face, z_face, diagonal, right, *rest):
    if second:
        image, step, sums, parts = rest
    else:
        image, sums, parts = rest
    cells, _, depth, systems = field.shape
    parts[...] = jnp.zeros_like(parts)

    def plane(x, has_below, has_above):
        energy = parts[0]
        curvature = parts[1]
        for y in range(cells):
            here = field[x, y]
            total = wide(diagonal[x, y], systems) * here
            if has_below:
                total -= wide(x_face[x - 1, y], systems) * field[x - 1, y]
            if has_above:
                total -= wide(x_face[x, y], systems) * field[x + 1, y]
            if y > 0:
                total -= wide(y_face[x, y - 1], systems) * field[x, y - 1]
            if y < cells - 1:
                total -= wide(y_face[x, y], systems) * field[x, y + 1]
            face = wide(z_face[x, y], systems)
            total -= face * pltpu.roll(here, depth - 1, 0)
            total -= pltpu.roll(face * here, 1, 0)
            if second:
                energy += fold_rows((right[x, y] - step[1:2] * image[x, y]) * here)
            else:
                image[x, y] = total
                energy += fold_rows(right[x, y] * here)
            curvature += fold_rows(here * total)
        parts[0] = energy
        parts[1] = curvature

    def middle(x, carry):
        plane(x, True, True)
        return carry

    plane(0, False, True)
    lax.fori_loop(1, cells - 1, middle, 0)
    plane(cells - 1, True, False)
    sums[...] = jnp.concatenate(
        [
            parts[0].sum(0, keepdims=True),
            parts[1].sum(0, keepdims=True),
            jnp.zeros((BOX - 2, systems), jnp.float32),
        ]
    )


def sweep(field, coefs, right, extra=()):
    systems = field.shape[-1]
    ins = (field, *coefs, right, *extra)
    outs = [f32(BOX, systems)]
    if not extra:
        outs = [f32(*field.shape)] + outs
    return pl.pallas_call(
        functools.partial(sweep_body, bool(extra)),
        in_specs=[VMEM] * len(ins),
        out_specs=[VMEM] * len(outs),
        out_shape=outs,
        scratch_shapes=[pltpu.VMEM((2, BOX, systems), jnp.float32)],
        compiler_params=limit(8),
        cost_estimate=cost(2000 * field.size, 16 * field.size),
        name="sweep",
    )(*ins)


def border_body(sizes, image_in, sums_in, xe, ye, ze, *rest):
    me = position()
    pairs = []
    for size in sizes:
        pairs.append([(rest[2 * k], rest[2 * k + 1]) for k in range(size)])
        rest = rest[2 * size :]
    leaf_w, leaf_s, dev_w, dev_s, image, device_in, up = rest
    cells, _, depth, systems = image.shape
    odd = [lax.rem(me[axis], 2) for axis in range(3)]

    def along(a, total):
        for axis, edge in ((0, xe), (1, ye)):
            for k, (own, halo) in enumerate(pairs[axis]):
                side = odd[axis] if k else 1 - odd[axis]
                spot = side * (cells - 1)
                term = wide(edge[side, a], systems) * halo[a]
                if axis == 0:
                    image[spot, a] -= term
                else:
                    image[a, spot] -= term
                total += own[a] * term
        for k, (own, halo) in enumerate(pairs[2]):
            side = odd[2] if k else 1 - odd[2]
            for here, spot in ((0, 0), (1, depth - 1)):
                chosen = jnp.where(side == here, 1.0, 0.0).astype(jnp.float32)
                term = wide(chosen * ze[here, a], systems) * halo[a]
                image[a, :, spot] -= term
                total += own[a] * term
        return total

    total = lax.fori_loop(0, cells, along, jnp.zeros((cells, systems), jnp.float32))
    rows = dev_w.shape[1]
    up[rows:] = sums_in[...]
    up[rows + 1 : rows + 2] = sums_in[1:2] - total.sum(0, keepdims=True)
    restrict_all(image, leaf_w, leaf_s, dev_w, dev_s, device_in, up.at[:rows])


def border(image, sums, edges, pairs, leaf_w, leaf_s, dev_w, dev_s):
    boxes, kept, _ = leaf_w.shape
    systems = image.shape[-1]
    flat = [array for found in pairs for pair in found for array in pair]
    ins = (image, sums, *edges, *flat, leaf_w, leaf_s, dev_w, dev_s)
    return pl.pallas_call(
        functools.partial(border_body, [len(found) for found in pairs]),
        in_specs=[VMEM] * len(ins),
        out_specs=[VMEM] * 3,
        out_shape=[
            f32(*image.shape),
            f32(boxes * kept, systems),
            f32(dev_w.shape[1] + BOX, systems),
        ],
        input_output_aliases={0: 0},
        compiler_params=limit(12),
        cost_estimate=restrict_cost(image, leaf_w, dev_w),
        name="border",
    )(*ins)


def across_body(sums_in, xe, ye, ze, x_own, y_own, z_own, x_halo, y_halo, z_halo, sums):
    cells, _, systems = x_halo.shape

    def along(a, total):
        total += wide(xe[0, a], systems) * x_own[a] * x_halo[a]
        total += wide(ye[0, a], systems) * y_own[a] * y_halo[a]
        return total + wide(ze[0, a], systems) * z_own[a] * z_halo[a]

    total = lax.fori_loop(0, cells, along, jnp.zeros((cells, systems), jnp.float32))
    sums[...] = sums_in[...]
    sums[1:2] = sums_in[1:2] - 2.0 * total.sum(0, keepdims=True)


def across(sums, edges, own, halo):
    ins = (sums, *edges, *own, *halo)
    return pl.pallas_call(
        across_body,
        in_specs=[VMEM] * len(ins),
        out_specs=VMEM,
        out_shape=f32(*sums.shape),
        compiler_params=limit(8),
        cost_estimate=cost(own[0].size * 20, own[0].size * 24),
        name="across",
    )(*ins)


def shifted(values, axis, step):
    count = lax.axis_size(axis)
    return lax.ppermute(values, axis, [(i, (i + step) % count) for i in range(count)])


def mirrored(sent, axis):
    count = lax.axis_size(axis)
    found = []
    for start in (0, 1) if count > 2 else (0,):
        pairs = []
        for i in range(count):
            j = ((i - start) ^ 1) + start
            pairs.append((i, j if 0 <= j < count else i))
        found.append((sent[start], lax.ppermute(sent[start], axis, pairs)))
    return found


def finish_body(first, corrected, sums, kept, out):
    energy, step = kept[0:1], kept[1:2]
    energy_new, curvature_new = sums[0:1], sums[1:2]
    mixing = energy_new / energy
    step_new = energy_new / (curvature_new - mixing * energy_new / step)
    out[...] = (step + step_new * mixing) * first[...] + step_new * corrected[...]


def finish(first, corrected, sums, kept):
    cells = first.shape[0]
    plane = pl.BlockSpec((4, *first.shape[1:]), lambda i: (i, 0, 0, 0))
    whole = pl.BlockSpec(sums.shape, lambda i: (0, 0))
    return pl.pallas_call(
        finish_body,
        grid=(cells // 4,),
        in_specs=[plane, plane, whole, whole],
        out_specs=plane,
        out_shape=f32(*first.shape),
        compiler_params=limit(8),
        name="finish",
    )(first, corrected, sums, kept)


def local(
    right_side,
    conductivity,
    reaction,
    leaf_factor,
    leaf_weight,
    leaf_skeleton,
    device_factor,
    device_weight,
    device_skeleton,
    column_factor,
    column_weight,
    column_skeleton,
    top_factor,
):
    cells = right_side.shape[0]
    systems = right_side.shape[3]
    boxes = (cells // BOX) ** 3
    leaf_size = BOX**3
    count_x, count_y, count_z = (lax.axis_size(a) for a in ("gx", "gy", "gz"))
    leaf_f = leaf_factor.reshape(boxes, leaf_size, leaf_size)
    dev_f = device_factor[0, 0, 0]
    col_f = column_factor[0, 0]
    col_w = column_weight[0, 0]
    col_s = column_skeleton[0]
    dev_s = device_skeleton[0, 0]
    (
        right_side, leaf_w, leaf_s, dev_w, dev_s, conductivity,
        dev_f, col_f, col_w, col_s, reaction, device_in, device_up, *packed,
    ) = load(
        right_side,
        jnp.swapaxes(leaf_weight, -1, -2).reshape(boxes, -1, leaf_size),
        leaf_skeleton.reshape(boxes, 1, -1),
        device_weight[0, 0, 0],
        dev_s,
        conductivity,
        top_factor,
        (dev_f, col_f, col_w, col_s, reaction),
        count_x,
        count_y,
    )
    levels = (leaf_w, leaf_s, dev_w, dev_s)
    rows_mine = dev_w.shape[1]
    col_k = col_w.shape[1]
    part = systems // count_z
    if part % LANES:
        part = systems

    blocks = [packed[0]] + [shifted(packed[k], "gy", k) for k in range(1, count_y)]

    def precondition(field, device_in, device_up, cond, cat, between):
        found = [device_up] + [shifted(device_up, "gz", k) for k in range(1, count_z)]
        mine, column_in = column(part, rows_mine, found, col_w, col_s, cond)
        gathered = [mine] + [shifted(mine, "gx", k) for k in range(1, count_x)]
        coarse = (dev_f, device_in, col_f, column_in)
        if cat is None:
            leaf_near, dev_near, col_near, cat = near(
                field, leaf_f, 0, boxes, coarse=coarse, leaf=(leaf_w, leaf_s)
            )
        else:
            part_near, dev_near, col_near = near(field, leaf_f, 0, boxes // 2, coarse=coarse)
            (leaf_near,) = near(field, leaf_f, boxes // 2, boxes // 2, into=part_near)
        partial = top_level(blocks, gathered, dev_near, cond is None)
        total = partial[0]
        for k in range(1, count_y):
            total = total + shifted(partial[k], "gy", -k)
        parts = [total]
        if part < systems:
            parts += [shifted(total, "gz", k) for k in range(1, count_z)]
        extra, kept = between(found, gathered, partial[1])
        lifted = lift(
            parts, col_w, col_s, col_near,
            dev_w, dev_s, dev_near, cat, leaf_near, *extra,
        )
        return lifted, (kept, cat)

    def first_between(found, gathered, partial):
        counts = (count_x, count_y, count_z)
        out = coefficients(counts, rows_mine, conductivity, reaction, found, gathered, blocks, partial)
        return ((out[3],), ()), (out[:4], out[4:])

    def second_between(found, gathered, partial):
        return ((), (first,)), None

    def summed(values):
        for axis in ("gz", "gy", "gx"):
            values = values + sum(shifted(values, axis, k) for k in range(1, lax.axis_size(axis)))
        return values

    lifted, ((coefs, edges), cat) = precondition(
        right_side, device_in, device_up, conductivity, None, first_between
    )
    first, own = lifted[0], lifted[1:]
    pairs = [mirrored(own[2 * k : 2 * k + 2], axis) for k, axis in enumerate(("gx", "gy", "gz"))]
    image, sums = sweep(first, coefs, right_side)
    image, device_in, device_up = border(image, sums, edges, pairs, *levels)

    lifted, _ = precondition(image, device_in, device_up, None, cat, second_between)
    corrected, own, kept = lifted[0], lifted[1:7], lifted[7]
    halo = [shifted(top, axis, 1) for top, axis in zip(own[::2], ("gx", "gy", "gz"))]
    (sums,) = sweep(corrected, coefs, right_side, (image, kept))
    sums = summed(across(sums, edges, own[1::2], halo))
    return finish(first, corrected, sums, kept)


def solution(mesh):
    return jax.shard_map(
        local,
        mesh=mesh,
        in_specs=(
            P("gx", "gy", "gz", None),
            P("gx", "gy", "gz"),
            P("gx", "gy", "gz"),
            P("gx", "gy", "gz", None, None),
            P("gx", "gy", "gz", None, None),
            P("gx", "gy", "gz", None),
            P("gx", "gy", "gz", None, None),
            P("gx", "gy", "gz", None, None),
            P("gx", "gy", "gz", None),
            P("gx", "gy", "gz", None),
            P("gx", "gy", None, None),
            P("gx", "gy", None),
            P(("gx", "gy"), None),
        ),
        out_specs=P("gx", "gy", "gz", None),
        check_vma=False,
    )
```

```python
import functools

import jax
import jax.numpy as jnp
from jax import lax
from jax.experimental import pallas as pl
from jax.experimental.pallas import tpu as pltpu
from jax.sharding import PartitionSpec as P

BOX = 8
LANES = 128
MIB = 1 << 20
NEAR_SLOTS = 3
LOAD_MIB = 16

def halves(values):
    high = values.astype(jnp.bfloat16)
    return high, (values - high.astype(values.dtype)).astype(jnp.bfloat16)


def product(left, right, left_dim=1):
    left_high, left_low = left if isinstance(left, tuple) else halves(left)
    right_high, right_low = right if isinstance(right, tuple) else halves(right)

    def one(a, b):
        return lax.dot_general(
            a, b, (((left_dim,), (0,)), ((), ())), preferred_element_type=jnp.float32
        )

    rows = left_high.shape[1 - left_dim]
    both = one(jnp.concatenate([left_high, left_low], axis=1 - left_dim), right_high)
    return both[:rows] + (both[rows:] + one(left_high, right_low))


def folded(weight, skeleton, first=0):
    rows = lax.broadcasted_iota(jnp.int32, weight.shape, weight.ndim - 2) + first
    return weight + (rows == skeleton).astype(weight.dtype)


def folded_across(weight, skeleton):
    kept, rows = weight.shape
    shape = (kept, kept)
    diagonal = lax.broadcasted_iota(jnp.int32, shape, 0) == lax.broadcasted_iota(jnp.int32, shape, 1)
    spread_out = jnp.broadcast_to(skeleton.astype(jnp.float32), shape)
    place = jnp.where(diagonal, spread_out, 0.0).sum(1, keepdims=True)
    lane = lax.broadcasted_iota(jnp.int32, weight.shape, 1).astype(jnp.float32)
    return weight + (lane == place).astype(weight.dtype)


def box_place(index, per_side):
    return index // (per_side * per_side), index // per_side % per_side, index % per_side


def cost(flops, moved):
    return pl.CostEstimate(flops=flops, bytes_accessed=moved, transcendentals=0)


VMEM = pl.BlockSpec(memory_space=pltpu.VMEM)
HBM = pl.BlockSpec(memory_space=pltpu.HBM)


def f32(*shape):
    return jax.ShapeDtypeStruct(shape, jnp.float32)


def position():
    return tuple(lax.axis_index(axis) for axis in ("gx", "gy", "gz"))


def limit(mib):
    return pltpu.CompilerParams(vmem_limit_bytes=mib * MIB)


def box_cells(box, per_side):
    return tuple(pl.ds(pl.multiple_of(p * BOX, BOX), BOX) for p in box_place(box, per_side))


def restrict_all(field, leaf_w, leaf_s, dev_w, dev_s, device_in, device_up):
    boxes, kept, _ = leaf_w.shape
    systems = field.shape[-1]
    per_side = field.shape[0] // BOX

    def one_box(box, carry):
        values = field[box_cells(box, per_side)].reshape(-1, systems)
        rows = pl.ds(pl.multiple_of(box * kept, kept), kept)
        device_in[rows] = product(folded_across(leaf_w[box], leaf_s[box]), values)
        return carry

    lax.fori_loop(0, boxes, one_box, 0, unroll=2)
    device_up[...] = product(folded(dev_w[...], dev_s[...]), device_in[...], 0)


def load_body(count_x, count_y, *refs):
    me = position()
    sources, refs = refs[:12], refs[12:]
    field, leaf_w, leaf_s, dev_w, dev_s, cond, *others, device_in, up = refs[:13]
    blocks = refs[13 : 13 + count_y]
    top, sems = refs[13 + count_y :]
    cells = cond.shape[0]
    per_side = cells // BOX
    boxes, kept, _ = leaf_w.shape
    systems = field.shape[-1]
    rows = dev_w.shape[1]
    right, *rest = sources
    copies = []

    def bring(source, target):
        copy = pltpu.make_async_copy(source, target, sems.at[len(copies)])
        copy.start()
        copies.append(copy)
        return copy

    small = [bring(rest[0], leaf_w), bring(rest[1], leaf_s)]
    parts = []
    for a in range(per_side):
        for b in range(per_side):
            parts.append((slice(a * BOX, (a + 1) * BOX), slice(b * BOX, (b + 1) * BOX)))
    ahead = 2
    waits = [bring(right.at[part], field.at[part]) for part in parts[:ahead]]
    later = []
    for copy in small:
        copy.wait()
    for index, part in enumerate(parts):
        waits[index].wait()
        if index + ahead < len(parts):
            part_ahead = parts[index + ahead]
            waits.append(bring(right.at[part_ahead], field.at[part_ahead]))
        elif not later:
            later = [bring(*pair) for pair in zip(rest[2:], (dev_w, dev_s, cond, top, *others))]
        for c in range(per_side):
            box = index * per_side + c
            values = field[(*part, slice(c * BOX, (c + 1) * BOX))].reshape(-1, systems)
            device_in[box * kept : (box + 1) * kept] = product(
                folded_across(leaf_w[box], leaf_s[box]), values
            )
    for copy in later:
        copy.wait()
    up[:rows] = product(folded(dev_w[...], dev_s[...]), device_in[...], 0)
    put_faces(up, rows, *z_faces(cond))
    size = top.shape[0]
    for k, out in enumerate(blocks):
        column = lax.rem(me[1] + k, count_y)
        for p in range(count_x):
            lanes = pl.ds(pl.multiple_of((p * count_y + column) * size, size), size)
            out[p * size : (p + 1) * size] = top[:, lanes]
        put_faces(out, count_x * size, cond[:, 0], cond[:, cells - 1])


def load(right, leaf_w, leaf_s, dev_w, dev_s, cond, top, others, count_x, count_y):
    boxes, kept, _ = leaf_w.shape
    systems = right.shape[-1]
    cells = cond.shape[0]
    kept_arrays = (right, leaf_w, leaf_s, dev_w, dev_s, cond, *others)
    size = top.shape[0]
    return pl.pallas_call(
        functools.partial(load_body, count_x, count_y),
        in_specs=[HBM] * 12,
        out_specs=[VMEM] * (13 + count_y),
        out_shape=[jax.ShapeDtypeStruct(a.shape, a.dtype) for a in kept_arrays]
        + [f32(boxes * kept, systems), f32(dev_w.shape[1] + 2 * cells, systems)]
        + [f32(count_x * size + 2 * cells, size)] * count_y,
        scratch_shapes=[
            pltpu.VMEM(top.shape, jnp.float32),
            pltpu.SemaphoreType.DMA((11 + (cells // BOX) ** 2,)),
        ],
        compiler_params=limit(LOAD_MIB),
        cost_estimate=restrict_cost(right, leaf_w, dev_w),
        name="load",
    )(*(pltpu.with_memory_space_constraint(a, pltpu.HBM) for a in (right, leaf_w, leaf_s, dev_w, dev_s, cond, top, *others)))


def z_faces(cond):
    cells = cond.shape[0]
    lane = lax.broadcasted_iota(jnp.int32, (cells, cells), 1)
    faces = []
    for place in (0, cells - 1):
        face = jnp.zeros((cells, cells), jnp.float32)
        for x in range(cells):
            chosen = jnp.broadcast_to(cond[x][:, place : place + 1], face.shape)
            face = jnp.where(lane == x, chosen, face)
        faces.append(face)
    return faces


def put_faces(ref, row, low, top):
    cells = low.shape[0]
    ref[row:] = jnp.zeros_like(ref[row:])
    ref[row : row + cells, :cells] = low
    ref[row + cells : row + 2 * cells, :cells] = top


def restrict_cost(field, leaf_w, dev_w):
    return cost(6 * field.shape[-1] * (leaf_w.size + dev_w.size), 4 * field.size)


def column_body(part, rows, first, count, *refs):
    me = position()
    found = refs[:count]
    col_w, col_s = refs[count : count + 2]
    mine, column_in = refs[-2:]
    systems = column_in.shape[1]
    for k in range(count):
        place = lax.rem(me[2] + count - k, count)
        column_in[pl.ds(pl.multiple_of(place * rows, BOX), rows)] = found[k][:rows]
    if part < systems:
        lanes = pl.ds(pl.multiple_of(me[2] * part, LANES), part)
    else:
        lanes = slice(None)
    size = col_w.shape[1]
    mine[:size] = product(folded(col_w[...], col_s[...]), column_in[:, lanes], 0)
    if first:
        cond = refs[count + 2]
        put_faces(mine, size, cond[0], cond[cond.shape[0] - 1])
    else:
        mine[size:] = sum(f[rows:, lanes] for f in found)


def column(part, rows, found, col_w, col_s, cond):
    count = len(found)
    systems = found[0].shape[1]
    extra = () if cond is None else (cond,)
    tail = BOX if cond is None else 2 * cond.shape[0]
    return pl.pallas_call(
        functools.partial(column_body, part, rows, bool(extra), count),
        in_specs=[VMEM] * (count + 2 + len(extra)),
        out_specs=[VMEM] * 2,
        out_shape=[f32(col_w.shape[1] + tail, part), f32(count * rows, systems)],
        compiler_params=limit(8),
        cost_estimate=cost(6 * part * col_w.size, 8 * count * rows * systems),
        name="column",
    )(*found, col_w, col_s, *extra)


def top_body(count_x, count_y, summing, *refs):
    me = position()
    blocks = refs[:count_y]
    gathered = refs[count_y : count_y + count_x]
    outs = refs[count_y + count_x + 1 : -1]
    whole = refs[-1]
    size = blocks[0].shape[1]
    for k in range(count_x):
        place = lax.rem(me[0] + count_x - k, count_x)
        whole[pl.ds(pl.multiple_of(place * size, size), size)] = gathered[k][:size]
    right = halves(whole[...])
    for k in range(count_y):
        left = jnp.concatenate(
            [blocks[k][p * size : (p + 1) * size] for p in range(count_x)], axis=1
        )
        outs[k][:size] = product(left, right)
    if summing:
        total = sum(g[size:] for g in gathered)
        for k in range(count_y):
            outs[k][size:] = total


def top_level(blocks, gathered, after, summing):
    count_x, count_y = len(gathered), len(blocks)
    size = blocks[0].shape[1]
    part = gathered[0].shape[1]
    return pl.pallas_call(
        functools.partial(top_body, count_x, count_y, summing),
        in_specs=[VMEM] * (count_y + count_x + 1),
        out_specs=[VMEM] * count_y,
        out_shape=[f32(size + BOX * summing, part)] * count_y,
        scratch_shapes=[pltpu.VMEM((count_x * size, part), jnp.float32)],
        compiler_params=limit(8),
        cost_estimate=cost(6 * part * count_x * count_y * size * size, 4 * count_x * count_y * size * size),
        name="top",
    )(*blocks, *gathered, after)


def near_body(first, count, has_into, wants_cat, field, leaf_f, *refs):
    refs = refs[has_into:]
    if wants_cat:
        dev_f, device_in, col_f, column_in, leaf_w, leaf_s = refs[:6]
        leaf_near, dev_near, col_near, cat, slots, sems = refs[6:]
    elif not has_into:
        dev_f, device_in, col_f, column_in, leaf_near, dev_near, col_near, slots, sems = refs
    else:
        leaf_near, slots, sems = refs
    systems = field.shape[-1]
    per_side = field.shape[0] // BOX

    def copy(box, slot):
        return pltpu.make_async_copy(leaf_f.at[box], slots.at[slot], sems.at[slot])

    for k in range(min(NEAR_SLOTS, count)):
        copy(first + k, k).start()
    if not has_into:
        dev_near[...] = product(dev_f[...], device_in[...])
        col_near[...] = product(col_f[...], column_in[...])

    def one_box(step, carry):
        box = first + step
        slot = lax.rem(step, NEAR_SLOTS)
        copy(box, slot).wait()
        here = box_cells(box, per_side)
        values = field[here].reshape(-1, systems)
        result = product(slots[slot], values)
        leaf_near[here] = result.reshape(BOX, BOX, BOX, systems)
        if wants_cat:
            high, low = halves(folded_across(leaf_w[box], leaf_s[box]).T)
            cat[box] = jnp.concatenate([high, low, high], axis=1)

        @pl.when(step + NEAR_SLOTS < count)
        def _():
            copy(box + NEAR_SLOTS, slot).start()

        return carry

    lax.fori_loop(0, count, one_box, 0)


def near(field, leaf_f, first, count, into=None, coarse=(), leaf=()):
    _, leaf_size, _ = leaf_f.shape
    systems = field.shape[-1]
    extra = coarse + leaf if into is None else (into,)
    out_shape = [f32(*field.shape)]
    flops = count * leaf_size * leaf_size
    if into is None:
        out_shape += [f32(coarse[0].shape[0], systems), f32(coarse[2].shape[0], systems)]
        flops += coarse[0].size + coarse[2].size
    if leaf:
        boxes, kept, _ = leaf[0].shape
        out_shape.append(jax.ShapeDtypeStruct((boxes, leaf_size, 3 * kept), jnp.bfloat16))
    return pl.pallas_call(
        functools.partial(near_body, first, count, into is not None, bool(leaf)),
        in_specs=[VMEM, HBM] + [VMEM] * len(extra),
        out_specs=[VMEM] * len(out_shape),
        out_shape=out_shape,
        scratch_shapes=[
            pltpu.VMEM((NEAR_SLOTS, leaf_size, leaf_size), jnp.float32),
            pltpu.SemaphoreType.DMA((NEAR_SLOTS,)),
        ],
        input_output_aliases={} if into is None else {2: 0},
        compiler_params=limit(12),
        cost_estimate=cost(6 * systems * flops, 4 * count * leaf_size * leaf_size),
        name="near",
    )(field, leaf_f, *extra)


def lift_body(unread, update, count_z, *refs):
    me = position()
    parts, refs = refs[:count_z], refs[count_z:]
    col_w, col_s, col_near, dev_w, dev_s, dev_near, cat, leaf_near, *rest = refs
    rest = rest[unread:]
    if update:
        base, rest = rest[0], rest[1:]
        kept, coarse, top_out = rest[7:]
    else:
        coarse, top_out = rest[7:]
    out, *sent = rest[:7]
    size = col_w.shape[1]
    part = parts[0].shape[1]
    for k in range(count_z):
        lanes = lax.rem(me[2] + count_z - k, count_z) * part
        top_out[:, pl.ds(pl.multiple_of(lanes, LANES), part)] = parts[k][...]
    if update:
        energy = top_out[size : size + 1]
        step = energy / top_out[size + 1 : size + 2]
        kept[...] = jnp.zeros_like(kept)
        kept[0:1] = energy
        kept[1:2] = step
    boxes = cat.shape[0]
    cells = out.shape[0]
    systems = out.shape[-1]
    per_side = cells // BOX
    count = col_near.shape[0]
    first = me[2] * count
    col_v = folded(col_w[pl.ds(pl.multiple_of(first, BOX), count)], col_s[...], first)
    column_out = col_near[...] + product(col_v, top_out[:size])
    device_out = dev_near[...] + product(folded(dev_w[...], dev_s[...]), column_out)
    coarse[...] = device_out.reshape(coarse.shape)
    odd = [0 if update else lax.rem(me[axis], 2) for axis in range(3)]

    def one_box(box, carry):
        places = box_place(box, per_side)
        here = box_cells(box, per_side)
        high, low = halves(coarse[box])
        far = jnp.dot(
            cat[box], jnp.concatenate([high, high, low]), preferred_element_type=jnp.float32
        )
        values = leaf_near[here] + far.reshape(BOX, BOX, BOX, systems)
        if update:
            values = base[here] - step * values
        out[here] = values
        for axis in range(3):
            others = tuple(h for k, h in enumerate(here) if k != axis)
            for side, spot, at in ((0, 0, 0), (1, BOX - 1, per_side - 1)):
                for slot in (0, 1):
                    target = sent[2 * axis + slot]

                    def put(axis=axis, spot=spot, target=target, others=others):
                        target[others] = values[(slice(None),) * axis + (spot,)]

                    if update:
                        if slot == 1 - side:
                            pl.when(places[axis] == at)(put)
                    else:
                        wanted = odd[axis] == (1 - side if slot == 0 else side)
                        pl.when((places[axis] == at) & wanted)(put)
        return carry

    lax.fori_loop(0, boxes, one_box, 0, unroll=2)


def lift(parts, col_w, col_s, col_near, dev_w, dev_s, dev_near, cat, leaf_near, unread, update):
    boxes, _, width = cat.shape
    systems = leaf_near.shape[-1]
    out_shape = [f32(*leaf_near.shape)] + [f32(*leaf_near.shape[1:])] * 6
    if update:
        out_shape.append(f32(BOX, systems))
    return pl.pallas_call(
        functools.partial(lift_body, len(unread), bool(update), len(parts)),
        in_specs=[VMEM] * (len(parts) + 8 + len(unread) + len(update)),
        out_specs=[VMEM] * len(out_shape),
        out_shape=out_shape,
        scratch_shapes=[
            pltpu.VMEM((boxes, width // 3, systems), jnp.float32),
            pltpu.VMEM((parts[0].shape[0], systems), jnp.float32),
        ],
        compiler_params=limit(12),
        cost_estimate=cost(6 * systems * (cat.size // 3 + dev_w.size), 8 * leaf_near.size),
        name="lift",
    )(*parts, col_w, col_s, col_near, dev_w, dev_s, dev_near, cat, leaf_near, *unread, *update)


def spread(left):
    ones = jnp.ones((left.shape[1], LANES), jnp.bfloat16)
    total = None
    for _ in range(3):
        part = left.astype(jnp.bfloat16)
        left = left - part.astype(left.dtype)
        term = jnp.dot(part, ones, preferred_element_type=jnp.float32)
        total = term if total is None else total + term
    return total


def spread_rows(values):
    count, width = values.shape
    wanted = (count, width, LANES)
    shape = (count * width, width)
    repeated = jnp.concatenate(
        [jnp.broadcast_to(values[a : a + 1], (width, width)) for a in range(count)]
    )
    row = lax.rem(lax.broadcasted_iota(jnp.int32, shape, 0), width)
    lane = lax.broadcasted_iota(jnp.int32, shape, 1)
    return spread(jnp.where(row == lane, repeated, 0.0)).reshape(wanted)


def spread_columns(values):
    width, count = values.shape
    lane = lax.broadcasted_iota(jnp.int32, values.shape, 1)
    left = jnp.concatenate([jnp.where(lane == a, values, 0.0) for a in range(count)])
    return spread(left).reshape(count, width, LANES)


def coefs_body(counts, rows, cond, react, z_below, z_above, x_below, x_above, y_below, y_above, after, x_face, y_face, z_face, diag, xe, ye, ze, half):
    me = position()
    cells = cond.shape[0]
    col_k = x_below.shape[0] - 2 * cells
    top_rows = y_below.shape[0] - 2 * cells

    def fill(x, carry):
        half[x] = spread_rows(0.5 * cond[x])
        diag[x] = spread_rows(react[x])
        return carry

    lax.fori_loop(0, cells, fill, 0, unroll=4)
    place = lax.broadcasted_iota(jnp.int32, (cells, cells, LANES), 1)

    def faces(x, carry):
        here = half[x]
        along_y = here[:-1] + here[1:]
        along_z = jnp.where(place < cells - 1, here + pltpu.roll(here, cells - 1, 1), 0.0)
        y_face[x] = along_y
        z_face[x] = along_z
        nothing = jnp.zeros_like(here[:1])
        diag[x] = (
            diag[x]
            + along_z
            + pltpu.roll(along_z, 1, 1)
            + jnp.concatenate([along_y, nothing])
            + jnp.concatenate([nothing, along_y])
        )
        return carry

    lax.fori_loop(0, cells, faces, 0)

    def between(x, carry):
        face = half[x] + half[x + 1]
        x_face[x] = face
        diag[x] += face
        diag[x + 1] += face
        return carry

    lax.fori_loop(0, cells - 1, between, 0)

    last = cells - 1
    other = (
        (x_below[col_k + cells :, :cells], x_above[col_k : col_k + cells, :cells]),
        (y_below[top_rows + cells :, :cells], y_above[top_rows : top_rows + cells, :cells]),
        (z_below[rows + cells :, :cells], z_above[rows : rows + cells, :cells]),
    )
    own = ((cond[0], cond[last]), (cond[:, 0], cond[:, last]), z_faces(cond))
    for axis, edge in enumerate((xe, ye, ze)):
        for side, spot in ((0, 0), (1, last)):
            open_side = me[axis] > 0 if side == 0 else me[axis] < counts[axis] - 1
            mask = jnp.where(open_side, 1.0, 0.0).astype(jnp.float32)
            small = 0.5 * (own[axis][side] + mask * other[axis][side])
            face = spread_columns(small) if axis == 2 else spread_rows(small)
            edge[side] = mask * face
            if axis == 0:
                diag[spot] += face
            elif axis == 1:
                diag[:, spot] += face
            else:
                diag[:, :, spot] += face


def coefficients(counts, rows, cond, react, found, gathered, blocks, after):
    cells = cond.shape[0]
    ins = (cond, react, found[1], found[-1], gathered[1], gathered[-1], blocks[1], blocks[-1], after)
    cube = f32(cells, cells, cells, LANES)
    edge = f32(2, cells, cells, LANES)
    return pl.pallas_call(
        functools.partial(coefs_body, counts, rows),
        in_specs=[VMEM] * 9,
        out_specs=[VMEM] * 7,
        out_shape=[
            f32(cells - 1, cells, cells, LANES),
            f32(cells, cells - 1, cells, LANES),
            cube,
            cube,
            edge,
            edge,
            edge,
        ],
        scratch_shapes=[pltpu.VMEM(cube.shape, jnp.float32)],
        compiler_params=limit(12),
        cost_estimate=cost(4000 * cond.size * LANES, 16 * cond.size * LANES),
        name="coefs",
    )(*ins)


def wide(values, systems):
    return jnp.concatenate([values] * (systems // LANES), axis=-1)


def fold_rows(values):
    return values.reshape(-1, BOX, values.shape[-1]).sum(0)


def sweep_body(second, field, x_face, y_face, z_face, diagonal, right, *rest):
    if second:
        image, step, sums, parts = rest
    else:
        image, sums, parts = rest
    cells, _, depth, systems = field.shape
    parts[...] = jnp.zeros_like(parts)

    def plane(x, has_below, has_above):
        energy = parts[0]
        curvature = parts[1]
        for y in range(cells):
            here = field[x, y]
            total = wide(diagonal[x, y], systems) * here
            if has_below:
                total -= wide(x_face[x - 1, y], systems) * field[x - 1, y]
            if has_above:
                total -= wide(x_face[x, y], systems) * field[x + 1, y]
            if y > 0:
                total -= wide(y_face[x, y - 1], systems) * field[x, y - 1]
            if y < cells - 1:
                total -= wide(y_face[x, y], systems) * field[x, y + 1]
            face = wide(z_face[x, y], systems)
            total -= face * pltpu.roll(here, depth - 1, 0)
            total -= pltpu.roll(face * here, 1, 0)
            if second:
                energy += fold_rows((right[x, y] - step[1:2] * image[x, y]) * here)
            else:
                image[x, y] = total
                energy += fold_rows(right[x, y] * here)
            curvature += fold_rows(here * total)
        parts[0] = energy
        parts[1] = curvature

    def middle(x, carry):
        plane(x, True, True)
        return carry

    plane(0, False, True)
    lax.fori_loop(1, cells - 1, middle, 0)
    plane(cells - 1, True, False)
    sums[...] = jnp.concatenate(
        [
            parts[0].sum(0, keepdims=True),
            parts[1].sum(0, keepdims=True),
            jnp.zeros((BOX - 2, systems), jnp.float32),
        ]
    )


def sweep(field, coefs, right, extra=()):
    systems = field.shape[-1]
    ins = (field, *coefs, right, *extra)
    outs = [f32(BOX, systems)]
    if not extra:
        outs = [f32(*field.shape)] + outs
    return pl.pallas_call(
        functools.partial(sweep_body, bool(extra)),
        in_specs=[VMEM] * len(ins),
        out_specs=[VMEM] * len(outs),
        out_shape=outs,
        scratch_shapes=[pltpu.VMEM((2, BOX, systems), jnp.float32)],
        compiler_params=limit(8),
        cost_estimate=cost(2000 * field.size, 16 * field.size),
        name="sweep",
    )(*ins)


def border_body(sizes, image_in, sums_in, xe, ye, ze, *rest):
    me = position()
    pairs = []
    for size in sizes:
        pairs.append([(rest[2 * k], rest[2 * k + 1]) for k in range(size)])
        rest = rest[2 * size :]
    leaf_w, leaf_s, dev_w, dev_s, image, device_in, up = rest
    cells, _, depth, systems = image.shape
    odd = [lax.rem(me[axis], 2) for axis in range(3)]

    def along(a, total):
        for axis, edge in ((0, xe), (1, ye)):
            for k, (own, halo) in enumerate(pairs[axis]):
                side = odd[axis] if k else 1 - odd[axis]
                spot = side * (cells - 1)
                term = wide(edge[side, a], systems) * halo[a]
                if axis == 0:
                    image[spot, a] -= term
                else:
                    image[a, spot] -= term
                total += own[a] * term
        for k, (own, halo) in enumerate(pairs[2]):
            side = odd[2] if k else 1 - odd[2]
            for here, spot in ((0, 0), (1, depth - 1)):
                chosen = jnp.where(side == here, 1.0, 0.0).astype(jnp.float32)
                term = wide(chosen * ze[here, a], systems) * halo[a]
                image[a, :, spot] -= term
                total += own[a] * term
        return total

    total = lax.fori_loop(0, cells, along, jnp.zeros((cells, systems), jnp.float32))
    rows = dev_w.shape[1]
    up[rows:] = sums_in[...]
    up[rows + 1 : rows + 2] = sums_in[1:2] - total.sum(0, keepdims=True)
    restrict_all(image, leaf_w, leaf_s, dev_w, dev_s, device_in, up.at[:rows])


def border(image, sums, edges, pairs, leaf_w, leaf_s, dev_w, dev_s):
    boxes, kept, _ = leaf_w.shape
    systems = image.shape[-1]
    flat = [array for found in pairs for pair in found for array in pair]
    ins = (image, sums, *edges, *flat, leaf_w, leaf_s, dev_w, dev_s)
    return pl.pallas_call(
        functools.partial(border_body, [len(found) for found in pairs]),
        in_specs=[VMEM] * len(ins),
        out_specs=[VMEM] * 3,
        out_shape=[
            f32(*image.shape),
            f32(boxes * kept, systems),
            f32(dev_w.shape[1] + BOX, systems),
        ],
        input_output_aliases={0: 0},
        compiler_params=limit(12),
        cost_estimate=restrict_cost(image, leaf_w, dev_w),
        name="border",
    )(*ins)


def across_body(sums_in, xe, ye, ze, x_own, y_own, z_own, x_halo, y_halo, z_halo, sums):
    cells, _, systems = x_halo.shape

    def along(a, total):
        total += wide(xe[0, a], systems) * x_own[a] * x_halo[a]
        total += wide(ye[0, a], systems) * y_own[a] * y_halo[a]
        return total + wide(ze[0, a], systems) * z_own[a] * z_halo[a]

    total = lax.fori_loop(0, cells, along, jnp.zeros((cells, systems), jnp.float32))
    sums[...] = sums_in[...]
    sums[1:2] = sums_in[1:2] - 2.0 * total.sum(0, keepdims=True)


def across(sums, edges, own, halo):
    ins = (sums, *edges, *own, *halo)
    return pl.pallas_call(
        across_body,
        in_specs=[VMEM] * len(ins),
        out_specs=VMEM,
        out_shape=f32(*sums.shape),
        compiler_params=limit(8),
        cost_estimate=cost(own[0].size * 20, own[0].size * 24),
        name="across",
    )(*ins)


def shifted(values, axis, step):
    count = lax.axis_size(axis)
    return lax.ppermute(values, axis, [(i, (i + step) % count) for i in range(count)])


def mirrored(sent, axis):
    count = lax.axis_size(axis)
    found = []
    for start in (0, 1) if count > 2 else (0,):
        pairs = []
        for i in range(count):
            j = ((i - start) ^ 1) + start
            pairs.append((i, j if 0 <= j < count else i))
        found.append((sent[start], lax.ppermute(sent[start], axis, pairs)))
    return found


def finish_body(first, corrected, sums, kept, out):
    energy, step = kept[0:1], kept[1:2]
    energy_new, curvature_new = sums[0:1], sums[1:2]
    mixing = energy_new / energy
    step_new = energy_new / (curvature_new - mixing * energy_new / step)
    out[...] = (step + step_new * mixing) * first[...] + step_new * corrected[...]


def finish(first, corrected, sums, kept):
    cells = first.shape[0]
    plane = pl.BlockSpec((4, *first.shape[1:]), lambda i: (i, 0, 0, 0))
    whole = pl.BlockSpec(sums.shape, lambda i: (0, 0))
    return pl.pallas_call(
        finish_body,
        grid=(cells // 4,),
        in_specs=[plane, plane, whole, whole],
        out_specs=plane,
        out_shape=f32(*first.shape),
        compiler_params=limit(8),
        name="finish",
    )(first, corrected, sums, kept)


def local(
    right_side,
    conductivity,
    reaction,
    leaf_factor,
    leaf_weight,
    leaf_skeleton,
    device_factor,
    device_weight,
    device_skeleton,
    column_factor,
    column_weight,
    column_skeleton,
    top_factor,
):
    cells = right_side.shape[0]
    systems = right_side.shape[3]
    boxes = (cells // BOX) ** 3
    leaf_size = BOX**3
    count_x, count_y, count_z = (lax.axis_size(a) for a in ("gx", "gy", "gz"))
    leaf_f = leaf_factor.reshape(boxes, leaf_size, leaf_size)
    dev_f = device_factor[0, 0, 0]
    col_f = column_factor[0, 0]
    col_w = column_weight[0, 0]
    col_s = column_skeleton[0]
    dev_s = device_skeleton[0, 0]
    (
        right_side, leaf_w, leaf_s, dev_w, dev_s, conductivity,
        dev_f, col_f, col_w, col_s, reaction, device_in, device_up, *packed,
    ) = load(
        right_side,
        jnp.swapaxes(leaf_weight, -1, -2).reshape(boxes, -1, leaf_size),
        leaf_skeleton.reshape(boxes, 1, -1),
        device_weight[0, 0, 0],
        dev_s,
        conductivity,
        top_factor,
        (dev_f, col_f, col_w, col_s, reaction),
        count_x,
        count_y,
    )
    levels = (leaf_w, leaf_s, dev_w, dev_s)
    rows_mine = dev_w.shape[1]
    col_k = col_w.shape[1]
    part = systems // count_z
    if part % LANES:
        part = systems

    blocks = [packed[0]] + [shifted(packed[k], "gy", k) for k in range(1, count_y)]

    def precondition(field, device_in, device_up, cond, cat, between):
        found = [device_up] + [shifted(device_up, "gz", k) for k in range(1, count_z)]
        mine, column_in = column(part, rows_mine, found, col_w, col_s, cond)
        gathered = [mine] + [shifted(mine, "gx", k) for k in range(1, count_x)]
        coarse = (dev_f, device_in, col_f, column_in)
        if cat is None:
            leaf_near, dev_near, col_near, cat = near(
                field, leaf_f, 0, boxes, coarse=coarse, leaf=(leaf_w, leaf_s)
            )
        else:
            part_near, dev_near, col_near = near(field, leaf_f, 0, boxes // 2, coarse=coarse)
            (leaf_near,) = near(field, leaf_f, boxes // 2, boxes // 2, into=part_near)
        partial = top_level(blocks, gathered, dev_near, cond is None)
        extra, kept = between(found, gathered, partial[1])
        if kept is None:
            total, leaf_near = lax.optimization_barrier((partial[0], leaf_near))
        else:
            (coefs, edges) = kept
            total, diagonal = lax.optimization_barrier((partial[0], coefs[3]))
            kept = ((*coefs[:3], diagonal), edges)
            extra = ((diagonal,), ())
        for k in range(1, count_y):
            total = total + shifted(partial[k], "gy", -k)
        parts = [total]
        if part < systems:
            parts += [shifted(total, "gz", k) for k in range(1, count_z)]
        lifted = lift(
            parts, col_w, col_s, col_near,
            dev_w, dev_s, dev_near, cat, leaf_near, *extra,
        )
        return lifted, (kept, cat)

    def first_between(found, gathered, partial):
        counts = (count_x, count_y, count_z)
        out = coefficients(counts, rows_mine, conductivity, reaction, found, gathered, blocks, partial)
        return ((out[3],), ()), (out[:4], out[4:])

    def second_between(found, gathered, partial):
        return ((), (first,)), None

    def summed(values):
        for axis in ("gz", "gy", "gx"):
            values = values + sum(shifted(values, axis, k) for k in range(1, lax.axis_size(axis)))
        return values

    lifted, ((coefs, edges), cat) = precondition(
        right_side, device_in, device_up, conductivity, None, first_between
    )
    first, own = lifted[0], lifted[1:]
    pairs = [mirrored(own[2 * k : 2 * k + 2], axis) for k, axis in enumerate(("gx", "gy", "gz"))]
    image, sums = sweep(first, coefs, right_side)
    image, device_in, device_up = border(image, sums, edges, pairs, *levels)

    lifted, _ = precondition(image, device_in, device_up, None, cat, second_between)
    corrected, own, kept = lifted[0], lifted[1:7], lifted[7]
    halo = [shifted(top, axis, 1) for top, axis in zip(own[::2], ("gx", "gy", "gz"))]
    (sums,) = sweep(corrected, coefs, right_side, (image, kept))
    sums = summed(across(sums, edges, own[1::2], halo))
    return finish(first, corrected, sums, kept)


def solution(mesh):
    return jax.shard_map(
        local,
        mesh=mesh,
        in_specs=(
            P("gx", "gy", "gz", None),
            P("gx", "gy", "gz"),
            P("gx", "gy", "gz"),
            P("gx", "gy", "gz", None, None),
            P("gx", "gy", "gz", None, None),
            P("gx", "gy", "gz", None),
            P("gx", "gy", "gz", None, None),
            P("gx", "gy", "gz", None, None),
            P("gx", "gy", "gz", None),
            P("gx", "gy", "gz", None),
            P("gx", "gy", None, None),
            P("gx", "gy", None),
            P(("gx", "gy"), None),
        ),
        out_specs=P("gx", "gy", "gz", None),
        check_vma=False,
    )
```
